128 devices in a mesh: orb: 64 (over x, z, y), trial: 2 (over core).
Axes of the slice: x: 4, y: 4, z: 4, core: 2. Of those that a mesh axis runs over, the one named last changes fastest.
Arguments:
- trials: float32 [4, 64, 4096], P('trial', 'orb'), may hold values from -120 to 120
- orbitals: bfloat16 [128, 64, 4096], P('orb'), may hold values from -6 to 6
- potential: float32 [64, 4096], P('orb'), may hold values from 0.5 to 2
- coulomb: float32 [3, 64, 64], replicated, may hold values from -0.75 to 0.75
- energies: float32 [128], replicated, may hold values from -1.5 to -0.3
- frequencies: float32 [8], replicated, may hold values from 0.3 to 4
- orbital_ids: int32 [128], P('orb'), may hold values from 0 to 127, each once
- freq_index: int32 [128], P('orb'), may hold values from 0 to 7
Outputs:
- filtered: float32 [4, 64, 4096], P('trial', 'orb')
The draws below stay inside these ranges and needn't reach their ends.
All inputs are finite; a program needn't handle non-finite values.
Results may differ from the reference program's by a relative error of at most 0.0003.
Values sent between devices are 32-bit elements; how exact they have to be, the bound alone decides.
A program may use at most 64 MiB of HBM per device.

```python
import math
import jax
import jax.numpy as jnp
from jax import lax

G = 64
NFREQ = 8
ITERS = 3
ORBS = 128
NTRIAL = 4


def draw_trials(key, part):
    draw_keys = jax.random.split(key, 2)
    shape_full = (NTRIAL, G, G * G)
    plane_scale = (10.0 ** (jnp.arange(G, dtype=jnp.float32) / (G - 1)))[None, :, None]
    cell_scale = jnp.exp(jax.random.uniform(draw_keys[1], shape_full, jnp.float32, 0.0, jnp.log(3.0)))
    base_values = jnp.clip(jax.random.normal(draw_keys[0], shape_full, jnp.float32), -4.0, 4.0)
    return base_values * plane_scale * cell_scale


def with_ends(values, key, low, top_value):
    dims = values.shape
    index_at = [jax.random.randint(jax.random.fold_in(key, axis), (), 0, dims[axis]) for axis in range(len(dims))]
    values = values.at[tuple(index_at)].set(low)
    longest = dims.index(max(dims))
    index_at[longest] = (index_at[longest] + 1) % dims[longest]
    return values.at[tuple(index_at)].set(top_value)


def block_levels(rng, shape, pieces, smallest, high):
    def one(axis_at, blocks):
        steps = jax.random.uniform(jax.random.fold_in(jax.random.fold_in(rng, 6), axis_at), (blocks,), jnp.float32, smallest / len(pieces), high / len(pieces))
        return jnp.repeat(jnp.exp(steps), shape[axis_at] // blocks).reshape((-1,) + (1,) * (len(shape) - axis_at - 1))

    level = one(*pieces[0])
    for cut in pieces[1:]:
        level = level * one(*cut)
    return level


def scatter_about(own_key, shape, width, most, cuts=(), kind=jnp.bfloat16):
    array = width * jax.random.normal(own_key, shape, jnp.float32)
    if cuts:
        array = array * block_levels(own_key, shape, cuts, -0.22, 0.18)
    return jnp.clip(array, -most, most).astype(kind)


def setup_inputs(seed: int = 0) -> dict:
    seeds = jax.random.split(jax.random.key(seed), 9)
    return {
        "trials": draw_trials(jax.random.fold_in(seeds[8], 71), 0),
        "orbitals": scatter_about(seeds[1], (ORBS, G, G * G), 1.0, 6.0, ((0, 64),)),
        "potential": jnp.clip(0.5 + 1.5 * jax.random.uniform(seeds[2], (G, G * G), jnp.float32) ** block_levels(seeds[2], (G, G * G), ((0, 64),), -0.2, 0.2), 0.5, 2.0),
        "coulomb": scatter_about(seeds[3], (3, G, G), G ** -0.5, 0.75, (), jnp.float32),
        "energies": jnp.clip(jax.random.uniform(seeds[4], (ORBS,), jnp.float32, -1.5, -0.3), -1.5, -0.3),
        "frequencies": jnp.clip(jnp.exp(jax.random.uniform(seeds[5], (NFREQ,), jnp.float32, math.log(0.3), math.log(4.0))), 0.3, 4.0),
        "orbital_ids": jax.random.permutation(seeds[6], ORBS).astype(jnp.int32),
        "freq_index": with_ends(jax.random.randint(seeds[7], (ORBS,), 0, NFREQ), jax.random.fold_in(seeds[7], 1), 0, NFREQ - 1).astype(jnp.int32),
    }


def orbital_shifts(orbital_ids, freq_index, energies, frequencies):
    energy_slots = lax.broadcasted_iota(jnp.int32, (1, energies.shape[0]), 1)
    picked_energy = lax.optimization_barrier(jnp.sum(jnp.where(orbital_ids[:, None] == energy_slots, energies[None, :], 0.0), axis=1))
    freq_slots = lax.broadcasted_iota(jnp.int32, (1, frequencies.shape[0]), 1)
    picked_freq = lax.optimization_barrier(jnp.sum(jnp.where(freq_index[:, None] == freq_slots, frequencies[None, :], 0.0), axis=1))
    return picked_freq - picked_energy

def neighbour_sum(grid_field):
    grid_width = grid_field.shape[-2]
    z_index = lax.broadcasted_iota(jnp.int32, (1, grid_field.shape[-1]), 1) % grid_width
    zero_cells = jnp.zeros_like(grid_field[..., :1])
    upper_z = jnp.where(z_index == grid_width - 1, 0.0, jnp.concatenate([grid_field[..., 1:], zero_cells], axis=-1))
    lower_z = jnp.where(z_index == 0, 0.0, jnp.concatenate([zero_cells, grid_field[..., :-1]], axis=-1))
    zero_line = jnp.zeros_like(grid_field[..., :grid_width])
    upper_y = jnp.concatenate([grid_field[..., grid_width:], zero_line], axis=-1)
    lower_y = jnp.concatenate([zero_line, grid_field[..., :-grid_width]], axis=-1)
    zero_plane = jnp.zeros_like(grid_field[..., :1, :])
    upper_x = jnp.concatenate([grid_field[..., 1:, :], zero_plane], axis=-2)
    lower_x = jnp.concatenate([zero_plane, grid_field[..., :-1, :]], axis=-2)
    return upper_z + lower_z + upper_y + lower_y + upper_x + lower_x

def apply_shifted(grid_field, potential, level_shift):
    return (3.0 + potential + level_shift) * grid_field - 0.5 * neighbour_sum(grid_field)

def cell_inner(left_field, right_field):
    return lax.optimization_barrier(jnp.sum(left_field * right_field, axis=(1, 2)))[:, None, None]

def sternheimer(source, potential, level_shift):
    iterate = jnp.zeros_like(source)
    residual = source
    direction = source
    norm_now = cell_inner(residual, residual)
    for sweep_index in range(ITERS):
        mapped = apply_shifted(direction, potential, level_shift)
        step_size = norm_now / cell_inner(direction, mapped)
        iterate = iterate + step_size * direction
        residual = residual - step_size * mapped
        norm_next = cell_inner(residual, residual)
        direction = residual + norm_next / norm_now * direction
        norm_now = norm_next
    return iterate

def orbital_response(whole, orbitals, potential, shifts):

    def one_orbital(accumulated, scanned):
        orbital, level_shift = scanned
        density = orbital.astype(jnp.float32)[None]
        solved = sternheimer(density * whole, potential, level_shift)
        return (accumulated - density * solved, None)
    result, unused = lax.scan(one_orbital, jnp.zeros_like(whole), (orbitals, shifts))
    return result

def coulomb_full(grid_field, factors):
    trial_count = grid_field.shape[0]
    grid_width = grid_field.shape[1]
    cube_view = grid_field.reshape(trial_count, grid_width, grid_width, grid_width)
    cube_view = jnp.einsum('cz,txyz->txyc', factors[2], cube_view, precision=lax.Precision.HIGHEST)
    cube_view = jnp.einsum('by,txyc->txbc', factors[1], cube_view, precision=lax.Precision.HIGHEST)
    cube_view = jnp.einsum('ax,txbc->tabc', factors[0], cube_view, precision=lax.Precision.HIGHEST)
    return cube_view.reshape(trial_count, grid_width, grid_width * grid_width)

def reference(trials, orbitals, potential, coulomb, energies, frequencies, orbital_ids, freq_index):
    shifts = orbital_shifts(orbital_ids, freq_index, energies, frequencies)
    mapped = coulomb_full(orbital_response(trials, orbitals, potential, shifts), coulomb)
    squares = cell_inner(trials, trials)
    center = cell_inner(trials, mapped) / squares
    spread = jnp.sqrt(cell_inner(mapped, mapped) / squares)
    first = (mapped - center * trials) / spread
    second_mapped = coulomb_full(orbital_response(first, orbitals, potential, shifts), coulomb)
    second = 2.0 * (second_mapped - center * first) / spread - trials
    columns = second.reshape(second.shape[0], -1)
    gram_matrix = jnp.dot(columns, columns.T, precision=lax.Precision.HIGHEST) / float(G ** 3)
    lower = jnp.linalg.cholesky(gram_matrix)
    identity = jnp.eye(gram_matrix.shape[0], dtype=gram_matrix.dtype)
    inverse = lax.linalg.triangular_solve(lower, identity, left_side=True, lower=True)
    return jnp.dot(inverse, columns, precision=lax.Precision.HIGHEST).reshape(second.shape)
```

```python
import jax
import jax.numpy as jnp
from jax import lax
from jax.experimental import pallas as pl
from jax.experimental.pallas import tpu as pltpu
from jax.sharding import PartitionSpec as P

G = 64
L = 128
MESH = pl.DeviceIdType.MESH
HIGHEST = lax.Precision.HIGHEST
F32 = jnp.float32
BF16 = jnp.bfloat16
ALL = slice(None)

DIMS = ("x", "z", "y")
STRIDE = {"x": 16, "z": 4, "y": 1}

GROUP = 80
MID = 1.25
EXTRA = 16
SUMS = 8

FIRST_COLORS = (
    (("y", "z", "x"), pl.ds(0, 32)),
    (("z", "x", "y"), pl.ds(32, 24)),
    (("x", "y", "z"), pl.ds(56, 24)),
)
SECOND_COLORS = (
    (("y", "z", "x"), pl.ds(0, 24)),
    (("z", "x", "y"), pl.ds(24, 24)),
    (("x", "y", "z"), pl.ds(48, 24)),
)
SUM_COLORS = (
    (("y", "z", "x"), pl.ds(0, 24)),
    (("z", "x", "y"), pl.ds(24, 24)),
    (("x", "y", "z"), pl.ds(48, 16)),
)


class Place:
    def __init__(self):
        self.orb = lax.axis_index("orb")
        self.trial = lax.axis_index("trial")
        self.at = {
            a: lax.rem(lax.div(self.orb, jnp.int32(STRIDE[a])), jnp.int32(4)) for a in DIMS
        }

    def step(self, axis, by):
        return lax.rem(self.at[axis] + jnp.int32(by % 4), jnp.int32(4))

    def peer(self, axis, by):
        return (self.orb + (self.step(axis, by) - self.at[axis]) * STRIDE[axis], self.trial)

    def partner(self):
        return (self.orb, 1 - self.trial)

    def own(self, ref):
        return ref.at[self.at["x"], self.at["z"], self.at["y"]]

    def region(self, ref, order, phase, index, rows, half=None):
        spec = dict(self.at)
        for a in order[:phase]:
            spec[a] = ALL
        if half is not None:
            spec[order[0]] = pl.ds(2 * half, 2)
        spec[order[phase]] = index
        return ref.at[spec["x"], spec["z"], spec["y"], rows]


def remote(src, dst, send_sem, recv_sem, device):
    copy = pltpu.make_async_remote_copy(
        src_ref=src,
        dst_ref=dst,
        send_sem=send_sem,
        recv_sem=recv_sem,
        device_id=device,
        device_id_type=MESH,
    )
    copy.start()
    return copy


def gather(me, full, colors, send_sem, recv_sem, meanwhile=None):
    sends = []
    for phase in range(3):
        near = []
        for c, (order, rows) in enumerate(colors):
            axis = order[phase]
            mine = me.region(full, order, phase, me.at[axis], rows)
            copies = [
                remote(mine, mine, send_sem.at[c, phase, k], recv_sem.at[c, phase, k], me.peer(axis, by))
                for k, by in enumerate((1, -1, 2) if phase == 0 else (1, -1))
            ]
            near.append(copies)
            sends += copies
        if phase == 0:
            if meanwhile is not None:
                meanwhile()
            for copies in near:
                for copy in copies:
                    copy.wait_recv()
            continue
        far = []
        for c, (order, rows) in enumerate(colors):
            axis = order[phase]
            for half, by in ((0, 1), (1, -1)):
                near[c][half].wait_recv()
                onward = me.region(full, order, phase, me.step(axis, -by), rows, half)
                k = 2 + half
                far.append(
                    remote(onward, onward, send_sem.at[c, phase, k], recv_sem.at[c, phase, k], me.peer(axis, by))
                )
        for copy in far:
            copy.wait_recv()
        sends += far
    return sends


def landing_shapes(colors):
    shapes = []
    for order, rows in colors:
        for phase in (2, 1):
            kept = [a for a in DIMS if a in order[:phase]]
            lead = tuple(2 if a == order[0] else 4 for a in kept)
            shapes.append(pltpu.VMEM((6, *lead, rows.size, L), F32))
        shapes.append(pltpu.VMEM((3, rows.size, L), F32))
    return shapes


def scatter_sums(me, part, landing, colors, send_sem, recv_sem):
    sends = []
    for phase in (2, 1):
        started = []
        for c, (order, rows) in enumerate(colors):
            axis = order[phase]
            land = landing[3 * c + 2 - phase]
            started.append(
                [
                    remote(
                        me.region(part, order, phase, me.step(axis, 2), rows, half),
                        land.at[half],
                        send_sem.at[c, phase, half],
                        recv_sem.at[c, phase, half],
                        me.peer(axis, by),
                    )
                    for half, by in ((0, 1), (1, -1))
                ]
            )
        for c, (order, rows) in enumerate(colors):
            axis = order[phase]
            land = landing[3 * c + 2 - phase]
            for k, half, by in ((2, 1, 1), (3, 0, -1)):
                started[c].append(
                    remote(
                        me.region(part, order, phase, me.step(axis, by), rows, half),
                        land.at[k],
                        send_sem.at[c, phase, k],
                        recv_sem.at[c, phase, k],
                        me.peer(axis, by),
                    )
                )
        for c, (order, rows) in enumerate(colors):
            axis = order[phase]
            land = landing[3 * c + 2 - phase]
            for k, half, by in ((4, 0, 1), (5, 1, -1)):
                started[c][half].wait_recv()
                onward = me.region(part, order, phase, me.step(axis, by), rows, half)
                onward[...] = onward[...] + land[half]
                started[c].append(
                    remote(
                        onward,
                        land.at[k],
                        send_sem.at[c, phase, k],
                        recv_sem.at[c, phase, k],
                        me.peer(axis, by),
                    )
                )
        for c, (order, rows) in enumerate(colors):
            axis = order[phase]
            land = landing[3 * c + 2 - phase]
            for copy in started[c][2:]:
                copy.wait_recv()
            for half, (one, other) in enumerate(((3, 4), (2, 5))):
                mine = me.region(part, order, phase, me.at[axis], rows, half)
                mine[...] = mine[...] + (land[one] + land[other])
            sends += started[c]
    started = []
    for c, (order, rows) in enumerate(colors):
        land = landing[3 * c + 2]
        started.append(
            [
                remote(
                    me.region(part, order, 0, me.step(order[0], by), rows),
                    land.at[by - 1],
                    send_sem.at[c, 0, by],
                    recv_sem.at[c, 0, by],
                    me.peer(order[0], by),
                )
                for by in (1, 2, 3)
            ]
        )
    for c, (order, rows) in enumerate(colors):
        land = landing[3 * c + 2]
        for copy in started[c]:
            copy.wait_recv()
        mine = me.region(part, order, 0, me.at[order[0]], rows)
        mine[...] = mine[...] + ((land[0] + land[1]) + land[2])
        sends += started[c]
    return sends


def lanes():
    return lax.broadcasted_iota(jnp.int32, (1, L), 1)


def swap(values):
    return pltpu.roll(values, G, 1)


def halves(values):
    low = lanes() < G
    first = jnp.sum(jnp.where(low, values, 0.0), axis=1, keepdims=True)
    second = jnp.sum(jnp.where(low, 0.0, values), axis=1, keepdims=True)
    return jnp.where(low, first, second)


def fold(values):
    t = [values[8 * k : 8 * k + 8] for k in range(8)]
    return ((t[0] + t[1]) + (t[2] + t[3])) + ((t[4] + t[5]) + (t[6] + t[7]))


def column(values):
    return jnp.sum(values, axis=0, keepdims=True)


def step_weights(m, shift):
    a = [m[k + 1] + shift * m[k] for k in range(5)]
    low10 = a[1] / a[0]
    low20 = a[2] / a[0]
    pivot1 = a[2] - low10 * a[1]
    some = pivot1 > 1e-6 * a[2]
    cross = a[3] - low10 * a[2]
    low21 = jnp.where(some, cross / pivot1, 0.0)
    pivot2 = a[4] - low20 * a[2] - low21 * cross
    more = some & (pivot2 > 1e-6 * a[4])
    y1 = m[1] - low10 * m[0]
    y2 = m[2] - low20 * m[0] - low21 * y1
    c2 = jnp.where(more, y2 / pivot2, 0.0)
    c1 = jnp.where(some, y1 / pivot1, 0.0) - low21 * c2
    c0 = m[0] / a[0] - low10 * c1 - low20 * c2
    return 2.0 * c0, 2.0 * c1, 2.0 * c2


def respond(fields, dens, pot, shifts, kx, part, trial_lines):
    u0, u1, u2 = fields
    slots = range(dens.shape[0])
    low = lanes() % G == 0
    high = lanes() % G == G - 1

    def begin(y, _):
        v = trial_lines(y)
        for s in slots:
            u0[s, y + 1, 8:72] = v * dens[s, y]
        return 0

    lax.fori_loop(0, G, begin, 0)

    def centred(u, s, y, diagonal):
        c = u[s, y + 1, 8:72]
        along_z = jnp.where(high, 0.0, pltpu.roll(c, L - 1, 1)) + jnp.where(low, 0.0, pltpu.roll(c, 1, 1))
        along_y = u[s, y, 8:72] + u[s, y + 2, 8:72]
        along_x = u[s, y + 1, 7:71] + u[s, y + 1, 9:73]
        return c, diagonal * c - (along_z + along_y + along_x)

    zero = jnp.zeros((8, L), F32)

    def first_power(y, sums):
        diagonal = pot[y]
        out = []
        for s in slots:
            c, q = centred(u0, s, y, diagonal)
            u1[s, y + 1, 8:72] = q
            a = sums[s]
            out.append((a[0] + fold(c * c), a[1] + fold(c * q), a[2] + fold(q * q)))
        return tuple(out)

    low_sums = lax.fori_loop(0, G, first_power, tuple((zero,) * 3 for _ in slots))

    def second_power(y, sums):
        diagonal = pot[y]
        out = []
        for s in slots:
            c, q = centred(u1, s, y, diagonal)
            u2[s, y + 1, 8:72] = q
            a = sums[s]
            out.append((a[0] + fold(c * q), a[1] + fold(q * q)))
        return tuple(out)

    high_sums = lax.fori_loop(0, G, second_power, tuple((zero,) * 2 for _ in slots))

    def third_power(y, sums):
        diagonal = pot[y]
        out = []
        for s in slots:
            c = u2[s, y + 1, 8:72]
            ahead = jnp.where(high, 0.0, pltpu.roll(c, L - 1, 1)) + u2[s, y + 2, 8:72] + u2[s, y + 1, 9:73]
            out.append(sums[s] + fold(c * (diagonal * c - (ahead + ahead))))
        return tuple(out)

    top_sums = lax.fori_loop(0, G, third_power, tuple(zero for _ in slots))

    weights = []
    for s in slots:
        moments = [halves(column(t)) for t in (*low_sums[s], *high_sums[s], top_sums[s])]
        weights.append(step_weights(moments, shifts[s]))

    rows = part.reshape(G * G, L)

    def finish(y, _):
        total = None
        for s in slots:
            w = [c * u[s, y + 1, 8:72] for c, u in zip(weights[s], (u0, u1, u2))]
            term = (w[0] + w[1] + w[2]) * dens[s, y]
            total = term if total is None else total + term
        total = -total
        upper = total.astype(BF16)
        lower = (total - upper.astype(F32)).astype(BF16)
        stacked = jnp.concatenate([upper, upper, lower], axis=0)
        rows[pl.ds(y, G, stride=G), :] = jnp.dot(kx, stacked, preferred_element_type=F32)
        return 0

    lax.fori_loop(0, G, finish, 0)


def kernel(
    energies,
    frequencies,
    orbital_ids,
    freq_index,
    trials,
    orbitals,
    potential,
    coulomb,
    out,
    full,
    mapped,
    pot_other,
    dens,
    pot,
    u0,
    u1,
    u2,
    part,
    other,
    small,
    first_send,
    first_recv,
    second_send,
    second_recv,
    sum_send,
    sum_recv,
    pair_send,
    pair_recv,
    small_send,
    small_recv,
    *landing,
):
    me = Place()
    slots = range(dens.shape[0])
    half = lanes() < G

    barrier = pltpu.get_barrier_semaphore()
    peers = [me.peer(a, by) for a in DIMS for by in (1, 2, 3)] + [me.partner()]
    for peer in peers:
        pl.semaphore_signal(barrier, inc=1, device_id=peer, device_id_type=MESH)

    plane = me.own(full)
    for k in range(G // 2):
        a = trials[0, :, k * L : (k + 1) * L]
        b = trials[1, :, k * L : (k + 1) * L]
        plane[2 * k : 2 * k + 1, :] = jnp.where(half, a, swap(b))
        plane[2 * k + 1 : 2 * k + 2, :] = jnp.where(half, swap(a), b)
    for k in range(EXTRA):
        start = pl.multiple_of((me.trial * EXTRA + k) * L, L)
        plane[G + k : G + k + 1, :] = potential[:, pl.ds(start, L)]

    pl.semaphore_wait(barrier, len(peers))

    def prepare():
        def clear(y, _):
            for u in (u0, u1, u2):
                for s in slots:
                    u[s, y, 0:8] = jnp.zeros((8, L), F32)
                    u[s, y, 72:80] = jnp.zeros((8, L), F32)
            return 0

        for u in (u0, u1, u2):
            for s in slots:
                u[s, 0] = jnp.zeros((GROUP, L), F32)
                u[s, G + 1] = jnp.zeros((GROUP, L), F32)
        lax.fori_loop(1, G + 1, clear, 0)

        def spread_out(k, _):
            for s in slots:
                t = orbitals[s, :, pl.ds(pl.multiple_of(k * L, L), L)].astype(F32)
                turned = swap(t)
                dens[s, 2 * k] = jnp.where(half, t, turned)
                dens[s, 2 * k + 1] = jnp.where(half, turned, t)
            return 0

        lax.fori_loop(0, G // 2, spread_out, 0)

    sends = gather(me, full, FIRST_COLORS, first_send, first_recv, prepare)

    pot_lines = full.at[:, :, :, pl.ds(G, EXTRA)]
    pot_copy = remote(pot_lines, pot_other, pair_send.at[0], pair_recv.at[0], me.partner())

    full_rows = full.reshape(G * (G + EXTRA), L)
    other_rows = pot_other.reshape(G * EXTRA, L)
    mapped_rows = mapped.reshape(G * (G + SUMS), L)

    def level(j, base, t):
        turned = swap(t)
        y = 2 * (base + j)
        pot[y] = 2.0 * jnp.where(half, t, turned) - 2.0 * MID
        pot[y + 1] = 2.0 * jnp.where(half, turned, t) - 2.0 * MID

    def own_level(j, _):
        level(j, me.trial * EXTRA, full_rows[pl.ds(G + j, G, stride=G + EXTRA), :])
        return 0

    def other_level(j, _):
        level(j, (1 - me.trial) * EXTRA, other_rows[pl.ds(j, G, stride=EXTRA), :])
        return 0

    lax.fori_loop(0, EXTRA, own_level, 0)
    pot_copy.wait_recv()
    lax.fori_loop(0, EXTRA, other_level, 0)

    shifts = []
    for s in slots:
        level_shift = frequencies[freq_index[s]] - energies[orbital_ids[s]]
        shifts.append(2.0 * (3.0 + level_shift) + 2.0 * MID)

    kx = coulomb[0]
    kx_upper = kx.astype(BF16)
    kx_lower = (kx - kx_upper.astype(F32)).astype(BF16)
    kx_parts = jnp.concatenate([kx_upper, kx_lower, kx_upper], axis=1)
    kz = jnp.concatenate([coulomb[2], coulomb[2]], axis=1)
    kz = jnp.concatenate([kz, kz], axis=0)
    same = (lax.broadcasted_iota(jnp.int32, (L, L), 0) < G) == (lax.broadcasted_iota(jnp.int32, (L, L), 1) < G)
    kz = jnp.where(same, kz, 0.0)

    def in_plane(values):
        turned = lax.dot_general(
            values, kz, (((1,), (1,)), ((), ())), precision=HIGHEST, preferred_element_type=F32
        )
        return jnp.dot(coulomb[1], turned, precision=HIGHEST, preferred_element_type=F32)

    fields = (u0, u1, u2)
    total = me.own(part)
    respond(
        fields, dens, pot, shifts, kx_parts, part, lambda y: full_rows[pl.ds(y, G, stride=G + EXTRA), :]
    )
    n = len(landing) // 2
    part_sends = scatter_sums(me, part, landing[:n], SUM_COLORS, sum_send.at[0], sum_recv.at[0])
    own_mapped = in_plane(total[...])
    own_trials = plane[0:G, :]
    sums = me.own(mapped)
    sums[0:G, :] = own_mapped
    sums[G : G + 1, :] = column(fold(own_trials * own_trials))
    sums[G + 1 : G + 2, :] = column(fold(own_trials * own_mapped))
    sums[G + 2 : G + 3, :] = column(fold(own_mapped * own_mapped))
    sums[G + 3 : G + SUMS, :] = jnp.zeros((SUMS - 3, L), F32)
    sends += gather(me, mapped, SECOND_COLORS, second_send, second_recv)

    all_sums = jnp.zeros((SUMS, L), F32)
    for x in range(4):
        for z in range(4):
            for y in range(4):
                all_sums = all_sums + mapped[x, z, y, G : G + SUMS, :]
    squares = halves(all_sums[0:1])
    center = halves(all_sums[1:2]) / squares
    spread = jnp.sqrt(halves(all_sums[2:3]) / squares)
    unspread = 1.0 / spread

    def first_lines(y):
        t = full_rows[pl.ds(y, G, stride=G + EXTRA), :]
        m = mapped_rows[pl.ds(y, G, stride=G + SUMS), :]
        return (m - center * t) * unspread

    for copy in part_sends:
        copy.wait_send()
    respond(fields, dens, pot, shifts, kx_parts, part, first_lines)
    part_sends = scatter_sums(me, part, landing[n:], SUM_COLORS, sum_send.at[1], sum_recv.at[1])
    own_first = (own_mapped - center * own_trials) * unspread
    second = 2.0 * (in_plane(total[...]) - center * own_first) * unspread - own_trials

    other[0] = second
    swap_copy = remote(other.at[0], other.at[1], pair_send.at[1], pair_recv.at[1], me.partner())
    swap_copy.wait_recv()
    theirs = other[1]
    is_first = me.trial == 0
    a = jnp.where(is_first, second, theirs)
    b = jnp.where(is_first, theirs, second)
    turned_a = swap(a)
    turned_b = swap(b)
    for k, product in enumerate((a * a, a * turned_a, b * b, b * turned_b, a * b, a * turned_b)):
        small[0, 0, k : k + 1] = column(fold(product))
    small[0, 0, 6:8] = jnp.zeros((2, L), F32)
    sends += part_sends + [pot_copy, swap_copy]
    for phase, axis in enumerate(DIMS):
        copies = [
            remote(
                small.at[phase, 0],
                small.at[phase, by],
                small_send.at[phase, by],
                small_recv.at[phase, by],
                me.peer(axis, by),
            )
            for by in (1, 2, 3)
        ]
        for copy in copies:
            copy.wait_recv()
        small[phase + 1, 0] = (small[phase, 0] + small[phase, 1]) + (small[phase, 2] + small[phase, 3])
        sends += copies
    block = small[3, 0] * (1.0 / float(G**3))

    def entry(row, upper):
        picked = jnp.where(half, 0.0, block[row : row + 1]) if upper else jnp.where(half, block[row : row + 1], 0.0)
        return jnp.sum(picked, axis=1, keepdims=True)

    gram = {
        (0, 0): entry(0, False),
        (1, 1): entry(0, True),
        (1, 0): entry(1, False),
        (2, 2): entry(2, False),
        (3, 3): entry(2, True),
        (3, 2): entry(3, False),
        (2, 0): entry(4, False),
        (3, 1): entry(4, True),
        (3, 0): entry(5, False),
        (2, 1): entry(5, True),
    }
    lower = {}
    for j in range(4):
        rest = gram[j, j]
        for k in range(j):
            rest = rest - lower[j, k] * lower[j, k]
        lower[j, j] = jnp.sqrt(rest)
        for i in range(j + 1, 4):
            rest = gram[i, j]
            for k in range(j):
                rest = rest - lower[i, k] * lower[j, k]
            lower[i, j] = rest / lower[j, j]
    nothing = jnp.zeros((1, 1), F32)
    inverse = {(i, j): nothing for i in range(4) for j in range(4)}
    for j in range(4):
        inverse[j, j] = 1.0 / lower[j, j]
        for i in range(j + 1, 4):
            rest = nothing
            for k in range(j, i):
                rest = rest - lower[i, k] * inverse[k, j]
            inverse[i, j] = rest / lower[i, i]
    copies = (
        jnp.where(half, a, turned_a),
        jnp.where(half, turned_a, a),
        jnp.where(half, b, turned_b),
        jnp.where(half, turned_b, b),
    )
    result = None
    for u in range(4):
        here = jnp.where(is_first, inverse[0, u], inverse[2, u])
        there = jnp.where(is_first, inverse[1, u], inverse[3, u])
        term = jnp.where(half, here, there) * copies[u]
        result = term if result is None else result + term
    other[2] = result
    for k in range(G // 2):
        a = other[2, 2 * k : 2 * k + 1, :]
        b = other[2, 2 * k + 1 : 2 * k + 2, :]
        out[0, :, k * L : (k + 1) * L] = jnp.where(half, a, swap(b))
        out[1, :, k * L : (k + 1) * L] = jnp.where(half, swap(a), b)
    for copy in sends:
        copy.wait_send()


def shards(trials, orbitals, potential, coulomb, energies, frequencies, orbital_ids, freq_index):
    slots = orbitals.shape[0]
    vmem = pl.BlockSpec(memory_space=pltpu.VMEM)
    smem = pl.BlockSpec(memory_space=pltpu.SMEM)
    dma = pltpu.SemaphoreType.DMA
    field = pltpu.VMEM((slots, G + 2, GROUP, L), F32)
    return pl.pallas_call(
        kernel,
        out_shape=jax.ShapeDtypeStruct(trials.shape, F32),
        in_specs=[smem] * 4 + [vmem] * 4,
        out_specs=vmem,
        scratch_shapes=[
            pltpu.VMEM((4, 4, 4, G + EXTRA, L), F32),
            pltpu.VMEM((4, 4, 4, G + SUMS, L), F32),
            pltpu.VMEM((4, 4, 4, EXTRA, L), F32),
            pltpu.VMEM((slots, G, G, L), F32),
            pltpu.VMEM((G, G, L), F32),
            field,
            field,
            field,
            pltpu.VMEM((4, 4, 4, G, L), F32),
            pltpu.VMEM((3, G, L), F32),
            pltpu.VMEM((4, 4, 8, L), F32),
            dma((3, 3, 4)),
            dma((3, 3, 4)),
            dma((3, 3, 4)),
            dma((3, 3, 4)),
            dma((2, 3, 3, 6)),
            dma((2, 3, 3, 6)),
            dma((2,)),
            dma((2,)),
            dma((3, 4)),
            dma((3, 4)),
            *landing_shapes(SUM_COLORS),
            *landing_shapes(SUM_COLORS),
        ],
        compiler_params=pltpu.CompilerParams(
            collective_id=0, has_side_effects=True, vmem_limit_bytes=60 * 2**20
        ),
        name="filter",
    )(energies, frequencies, orbital_ids, freq_index, trials, orbitals, potential, coulomb)


def solution(mesh):
    in_specs = (
        P("trial", "orb", None),
        P("orb", None, None),
        P("orb", None),
        P(),
        P(),
        P(),
        P("orb"),
        P("orb"),
    )
    return jax.shard_map(
        shards, mesh=mesh, in_specs=in_specs, out_specs=P("trial", "orb", None), check_vma=False
    )
```

```python
import jax
import jax.numpy as jnp
from jax import lax
from jax.experimental import pallas as pl
from jax.experimental.pallas import tpu as pltpu
from jax.sharding import PartitionSpec as P

G = 64
L = 128
MESH = pl.DeviceIdType.MESH
HIGHEST = lax.Precision.HIGHEST
F32 = jnp.float32
BF16 = jnp.bfloat16
ALL = slice(None)

DIMS = ("x", "z", "y")
STRIDE = {"x": 16, "z": 4, "y": 1}

GROUP = 80
LINES = 8
MID = 1.25
EXTRA = 16
SUMS = 8

FIRST_COLORS = (
    (("y", "z", "x"), pl.ds(0, 32)),
    (("z", "x", "y"), pl.ds(32, 24)),
    (("x", "y", "z"), pl.ds(56, 24)),
)
SECOND_COLORS = (
    (("y", "z", "x"), pl.ds(0, 24)),
    (("z", "x", "y"), pl.ds(24, 24)),
    (("x", "y", "z"), pl.ds(48, 24)),
)
SUM_COLORS = (
    (("y", "z", "x"), pl.ds(0, 24)),
    (("z", "x", "y"), pl.ds(24, 24)),
    (("x", "y", "z"), pl.ds(48, 16)),
)


class Place:
    def __init__(self):
        self.orb = lax.axis_index("orb")
        self.trial = lax.axis_index("trial")
        self.at = {
            a: lax.rem(lax.div(self.orb, jnp.int32(STRIDE[a])), jnp.int32(4)) for a in DIMS
        }

    def step(self, axis, by):
        return lax.rem(self.at[axis] + jnp.int32(by % 4), jnp.int32(4))

    def peer(self, axis, by):
        return (self.orb + (self.step(axis, by) - self.at[axis]) * STRIDE[axis], self.trial)

    def partner(self):
        return (self.orb, 1 - self.trial)

    def own(self, ref):
        return ref.at[self.at["x"], self.at["z"], self.at["y"]]

    def region(self, ref, order, phase, index, rows, half=None):
        spec = dict(self.at)
        for a in order[:phase]:
            spec[a] = ALL
        if half is not None:
            spec[order[0]] = pl.ds(2 * half, 2)
        spec[order[phase]] = index
        return ref.at[spec["x"], spec["z"], spec["y"], rows]


def remote(src, dst, send_sem, recv_sem, device):
    copy = pltpu.make_async_remote_copy(
        src_ref=src,
        dst_ref=dst,
        send_sem=send_sem,
        recv_sem=recv_sem,
        device_id=device,
        device_id_type=MESH,
    )
    copy.start()
    return copy


def gather(me, full, colors, send_sem, recv_sem, meanwhile=None):
    sends = []
    state = []
    for i, (order, rows) in enumerate(colors):
        state.append(Route(me, full, order, rows, send_sem.at[i], recv_sem.at[i], sends))
    for r in state:
        r.first = [r.send(r.planes(), k, 0, by) for k, by in enumerate((1, -1, 2))]
    for r in state:
        wait_all(r.first)
        r.second = [r.send(r.planes(a=ALL), 3 + k, 1, by) for k, by in enumerate((1, -1))]
        r.third = {0: r.outward(0)}
    if meanwhile is not None:
        meanwhile()
    for r in state:
        r.second_far = []
        for half, by in ((0, 1), (1, -1)):
            r.second[half].wait_recv()
            r.second_far.append(r.send(r.planes(a=half, b=-by), 5 + half, 1, by))
            r.third[-by] = r.outward(-by)
    for r in state:
        r.pass_on(0)
    for r in state:
        wait_all(r.second_far)
        r.third[2] = r.outward(2)
    for group in (-1, 1, 2):
        for r in state:
            r.pass_on(group)
    for r in state:
        wait_all(r.last)
    return sends


def wait_all(copies):
    for copy in copies:
        copy.wait_recv()


class Route:
    def __init__(self, me, ref, order, rows, send_sem, recv_sem, sends):
        self.me, self.ref, self.order, self.rows = me, ref, order, rows
        self.send_sem, self.recv_sem, self.sends = send_sem, recv_sem, sends
        self.last = []

    def planes(self, a=None, b=0, c=0):
        me, (da, db, dc) = self.me, self.order
        spec = {db: me.step(db, b), dc: me.step(dc, c)}
        if a is None:
            spec[da] = me.at[da]
        elif a is ALL:
            spec[da] = ALL
        else:
            spec[da] = pl.ds(2 * a, 2)
        return self.ref.at[spec["x"], spec["z"], spec["y"], self.rows]

    def send(self, src, k, axis, by, dst=None):
        copy = remote(
            src,
            src if dst is None else dst,
            self.send_sem.at[k],
            self.recv_sem.at[k],
            self.me.peer(self.order[axis], by),
        )
        self.sends.append(copy)
        return copy

    def slot(self, group):
        return 7 + 4 * (group % 4)

    def outward(self, group):
        k = self.slot(group)
        return [self.send(self.planes(a=ALL, b=group), k + n, 2, by) for n, by in enumerate((1, -1))]

    def pass_on(self, group):
        k = self.slot(group) + 2
        for half, by in ((0, 1), (1, -1)):
            self.third[group][half].wait_recv()
            self.last.append(self.send(self.planes(a=half, b=group, c=-by), k + half, 2, by))


def landing_shapes(colors):
    shapes = []
    for order, rows in colors:
        for phase in (2, 1):
            kept = [a for a in DIMS if a in order[:phase]]
            lead = tuple(2 if a == order[0] else 4 for a in kept)
            shapes.append(pltpu.VMEM((6, *lead, rows.size, L), F32))
        shapes.append(pltpu.VMEM((3, rows.size, L), F32))
    return shapes


def scatter_sums(me, part, landing, colors, send_sem, recv_sem):
    sends = []
    for phase in (2, 1):
        started = []
        for c, (order, rows) in enumerate(colors):
            axis = order[phase]
            land = landing[3 * c + 2 - phase]
            started.append(
                [
                    remote(
                        me.region(part, order, phase, me.step(axis, 2), rows, half),
                        land.at[half],
                        send_sem.at[c, phase, half],
                        recv_sem.at[c, phase, half],
                        me.peer(axis, by),
                    )
                    for half, by in ((0, 1), (1, -1))
                ]
            )
        for c, (order, rows) in enumerate(colors):
            axis = order[phase]
            land = landing[3 * c + 2 - phase]
            for k, half, by in ((2, 1, 1), (3, 0, -1)):
                started[c].append(
                    remote(
                        me.region(part, order, phase, me.step(axis, by), rows, half),
                        land.at[k],
                        send_sem.at[c, phase, k],
                        recv_sem.at[c, phase, k],
                        me.peer(axis, by),
                    )
                )
        for c, (order, rows) in enumerate(colors):
            axis = order[phase]
            land = landing[3 * c + 2 - phase]
            for k, half, by in ((4, 0, 1), (5, 1, -1)):
                started[c][half].wait_recv()
                onward = me.region(part, order, phase, me.step(axis, by), rows, half)
                onward[...] = onward[...] + land[half]
                started[c].append(
                    remote(
                        onward,
                        land.at[k],
                        send_sem.at[c, phase, k],
                        recv_sem.at[c, phase, k],
                        me.peer(axis, by),
                    )
                )
        for c, (order, rows) in enumerate(colors):
            axis = order[phase]
            land = landing[3 * c + 2 - phase]
            for copy in started[c][2:]:
                copy.wait_recv()
            for half, (one, other) in enumerate(((3, 4), (2, 5))):
                mine = me.region(part, order, phase, me.at[axis], rows, half)
                mine[...] = mine[...] + (land[one] + land[other])
            sends += started[c]
    started = []
    for c, (order, rows) in enumerate(colors):
        land = landing[3 * c + 2]
        started.append(
            [
                remote(
                    me.region(part, order, 0, me.step(order[0], by), rows),
                    land.at[by - 1],
                    send_sem.at[c, 0, by],
                    recv_sem.at[c, 0, by],
                    me.peer(order[0], by),
                )
                for by in (1, 2, 3)
            ]
        )
    for c, (order, rows) in enumerate(colors):
        land = landing[3 * c + 2]
        for copy in started[c]:
            copy.wait_recv()
        mine = me.region(part, order, 0, me.at[order[0]], rows)
        mine[...] = mine[...] + ((land[0] + land[1]) + land[2])
        sends += started[c]
    return sends


def lanes():
    return lax.broadcasted_iota(jnp.int32, (1, L), 1)


def swap(values):
    return pltpu.roll(values, G, 1)


def halves(values):
    low = lanes() < G
    first = jnp.sum(jnp.where(low, values, 0.0), axis=1, keepdims=True)
    second = jnp.sum(jnp.where(low, 0.0, values), axis=1, keepdims=True)
    return jnp.where(low, first, second)


def fold(values):
    t = [values[8 * k : 8 * k + 8] for k in range(8)]
    return ((t[0] + t[1]) + (t[2] + t[3])) + ((t[4] + t[5]) + (t[6] + t[7]))


def column(values):
    return jnp.sum(values, axis=0, keepdims=True)


def step_weights(m, shift):
    a = [m[k + 1] + shift * m[k] for k in range(5)]
    low10 = a[1] / a[0]
    low20 = a[2] / a[0]
    pivot1 = a[2] - low10 * a[1]
    some = pivot1 > 1e-6 * a[2]
    cross = a[3] - low10 * a[2]
    low21 = jnp.where(some, cross / pivot1, 0.0)
    pivot2 = a[4] - low20 * a[2] - low21 * cross
    more = some & (pivot2 > 1e-6 * a[4])
    y1 = m[1] - low10 * m[0]
    y2 = m[2] - low20 * m[0] - low21 * y1
    c2 = jnp.where(more, y2 / pivot2, 0.0)
    c1 = jnp.where(some, y1 / pivot1, 0.0) - low21 * c2
    c0 = m[0] / a[0] - low10 * c1 - low20 * c2
    return 2.0 * c0, 2.0 * c1, 2.0 * c2


def split(values):
    upper = values.astype(BF16)
    return upper, (values - upper.astype(F32)).astype(BF16)


def respond(fields, dens, pot, shifts, kx, part, trial_lines):
    u0, u1, u2, near_even, near_odd, stack_even, stack_odd = fields
    slots = range(dens.shape[0])
    lines = near_even.shape[1]
    chunks = G // lines
    row = lax.broadcasted_iota(jnp.int32, (2 * L, L), 0) % L
    col = lax.broadcasted_iota(jnp.int32, (2 * L, L), 1)
    beside = (jnp.abs(row - col) == 1) & ((row < G) == (col < G))
    beside = jnp.where(beside, 1.0, 0.0).astype(BF16)

    def begin(y, _):
        v = trial_lines(y)
        for s in slots:
            u0[s, y + 1, 8:72] = v * dens[s, y]
        return 0

    lax.fori_loop(0, G, begin, 0, unroll=4)

    def along_z(u, chunk, near):
        for k in range(lines):
            y = chunk * lines + k
            upper, lower = split(jnp.concatenate([u[s, y + 1, 8:72] for s in slots], axis=0))
            sums = jnp.dot(jnp.concatenate([upper, lower], axis=1), beside, preferred_element_type=F32)
            for s in slots:
                near[s, k] = sums[G * s : G * s + G]

    def sweep(u, at_line, sums):
        along_z(u, 0, near_even)

        def pair(j, sums):
            for near, ahead, chunk in ((near_even, near_odd, 2 * j), (near_odd, near_even, 2 * j + 1)):
                along_z(u, lax.rem(chunk + 1, jnp.int32(chunks)), ahead)
                for k in range(lines):
                    y = chunk * lines + k
                    diagonal = pot[y]
                    sums = tuple(at_line(s, y, diagonal, near[s, k], sums[s]) for s in slots)
            return sums

        return lax.fori_loop(0, chunks // 2, pair, sums)

    def centred(u, s, y, diagonal, near):
        c = u[s, y + 1, 8:72]
        along_y = u[s, y, 8:72] + u[s, y + 2, 8:72]
        along_x = u[s, y + 1, 7:71] + u[s, y + 1, 9:73]
        return c, diagonal * c - (near + (along_y + along_x))

    zero = jnp.zeros((8, L), F32)

    def first_power(s, y, diagonal, near, a):
        c, q = centred(u0, s, y, diagonal, near)
        u1[s, y + 1, 8:72] = q
        return a[0] + fold(c * c), a[1] + fold(c * q), a[2] + fold(q * q)

    low_sums = sweep(u0, first_power, tuple((zero,) * 3 for _ in slots))

    def second_power(s, y, diagonal, near, a):
        c, q = centred(u1, s, y, diagonal, near)
        u2[s, y + 1, 8:72] = q
        return a[0] + fold(c * q), a[1] + fold(q * q)

    high_sums = sweep(u1, second_power, tuple((zero,) * 2 for _ in slots))

    def third_power(s, y, diagonal, near, a):
        c = u2[s, y + 1, 8:72]
        ahead = u2[s, y + 2, 8:72] + u2[s, y + 1, 9:73]
        return a + fold(c * (diagonal * c - (near + (ahead + ahead))))

    top_sums = sweep(u2, third_power, tuple(zero for _ in slots))

    weights = []
    for s in slots:
        moments = [halves(column(t)) for t in (*low_sums[s], *high_sums[s], top_sums[s])]
        weights.append(step_weights(moments, shifts[s]))

    rows = part.reshape(G * G, L)

    def gathered(j, stack):
        for k in range(2):
            y = 2 * j + k
            total = None
            for s in slots:
                w = [c * u[s, y + 1, 8:72] for c, u in zip(weights[s], (u0, u1, u2))]
                term = (w[0] + w[1] + w[2]) * dens[s, y]
                total = term if total is None else total + term
            upper, lower = split(-total)
            stack[0:G, k * L : k * L + L] = upper
            stack[G : 2 * G, k * L : k * L + L] = upper
            stack[2 * G : 3 * G, k * L : k * L + L] = lower

    def mixed(j, stack):
        sums = jnp.dot(kx, stack[...], preferred_element_type=F32)
        for k in range(2):
            rows[pl.ds(2 * j + k, G, stride=G), :] = sums[:, k * L : k * L + L]

    gathered(0, stack_even)

    def finish(j, _):
        for stack, ahead, y_pair in ((stack_even, stack_odd, 2 * j), (stack_odd, stack_even, 2 * j + 1)):
            gathered(lax.rem(y_pair + 1, jnp.int32(G // 2)), ahead)
            mixed(y_pair, stack)
        return 0

    lax.fori_loop(0, G // 4, finish, 0)


def kernel(
    energies,
    frequencies,
    orbital_ids,
    freq_index,
    trials,
    orbitals,
    potential,
    coulomb,
    out,
    full,
    mapped,
    pot_other,
    dens,
    pot,
    u0,
    u1,
    u2,
    near_even,
    near_odd,
    stack_even,
    stack_odd,
    part,
    other,
    small,
    first_send,
    first_recv,
    second_send,
    second_recv,
    sum_send,
    sum_recv,
    pair_send,
    pair_recv,
    small_send,
    small_recv,
    *landing,
):
    me = Place()
    slots = range(dens.shape[0])
    half = lanes() < G

    barrier = pltpu.get_barrier_semaphore()
    peers = [me.peer(a, by) for a in DIMS for by in (1, 2, 3)] + [me.partner()]
    for peer in peers:
        pl.semaphore_signal(barrier, inc=1, device_id=peer, device_id_type=MESH)

    plane = me.own(full)
    for k in range(G // 2):
        a = trials[0, :, k * L : (k + 1) * L]
        b = trials[1, :, k * L : (k + 1) * L]
        plane[2 * k : 2 * k + 1, :] = jnp.where(half, a, swap(b))
        plane[2 * k + 1 : 2 * k + 2, :] = jnp.where(half, swap(a), b)
    for k in range(EXTRA):
        start = pl.multiple_of((me.trial * EXTRA + k) * L, L)
        plane[G + k : G + k + 1, :] = potential[:, pl.ds(start, L)]

    pl.semaphore_wait(barrier, len(peers))

    def prepare():
        def clear(y, _):
            for u in (u0, u1, u2):
                for s in slots:
                    u[s, y, 0:8] = jnp.zeros((8, L), F32)
                    u[s, y, 72:80] = jnp.zeros((8, L), F32)
            return 0

        for u in (u0, u1, u2):
            for s in slots:
                u[s, 0] = jnp.zeros((GROUP, L), F32)
                u[s, G + 1] = jnp.zeros((GROUP, L), F32)
        lax.fori_loop(1, G + 1, clear, 0)

        def spread_out(k, _):
            for s in slots:
                t = orbitals[s, :, pl.ds(pl.multiple_of(k * L, L), L)].astype(F32)
                turned = swap(t)
                dens[s, 2 * k] = jnp.where(half, t, turned)
                dens[s, 2 * k + 1] = jnp.where(half, turned, t)
            return 0

        lax.fori_loop(0, G // 2, spread_out, 0)

    sends = gather(me, full, FIRST_COLORS, first_send, first_recv, prepare)

    pot_lines = full.at[:, :, :, pl.ds(G, EXTRA)]
    pot_copy = remote(pot_lines, pot_other, pair_send.at[0], pair_recv.at[0], me.partner())

    full_rows = full.reshape(G * (G + EXTRA), L)
    other_rows = pot_other.reshape(G * EXTRA, L)
    mapped_rows = mapped.reshape(G * (G + SUMS), L)

    def level(j, base, t):
        turned = swap(t)
        y = 2 * (base + j)
        pot[y] = 2.0 * jnp.where(half, t, turned) - 2.0 * MID
        pot[y + 1] = 2.0 * jnp.where(half, turned, t) - 2.0 * MID

    def own_level(j, _):
        level(j, me.trial * EXTRA, full_rows[pl.ds(G + j, G, stride=G + EXTRA), :])
        return 0

    def other_level(j, _):
        level(j, (1 - me.trial) * EXTRA, other_rows[pl.ds(j, G, stride=EXTRA), :])
        return 0

    lax.fori_loop(0, EXTRA, own_level, 0)
    pot_copy.wait_recv()
    lax.fori_loop(0, EXTRA, other_level, 0)

    shifts = []
    for s in slots:
        level_shift = frequencies[freq_index[s]] - energies[orbital_ids[s]]
        shifts.append(2.0 * (3.0 + level_shift) + 2.0 * MID)

    kx = coulomb[0]
    kx_upper = kx.astype(BF16)
    kx_lower = (kx - kx_upper.astype(F32)).astype(BF16)
    kx_parts = jnp.concatenate([kx_upper, kx_lower, kx_upper], axis=1)
    kz = jnp.concatenate([coulomb[2], coulomb[2]], axis=1)
    kz = jnp.concatenate([kz, kz], axis=0)
    same = (lax.broadcasted_iota(jnp.int32, (L, L), 0) < G) == (lax.broadcasted_iota(jnp.int32, (L, L), 1) < G)
    kz = jnp.where(same, kz, 0.0)

    def in_plane(values):
        turned = lax.dot_general(
            values, kz, (((1,), (1,)), ((), ())), precision=HIGHEST, preferred_element_type=F32
        )
        return jnp.dot(coulomb[1], turned, precision=HIGHEST, preferred_element_type=F32)

    fields = (u0, u1, u2, near_even, near_odd, stack_even, stack_odd)
    total = me.own(part)
    respond(
        fields, dens, pot, shifts, kx_parts, part, lambda y: full_rows[pl.ds(y, G, stride=G + EXTRA), :]
    )
    n = len(landing) // 2
    part_sends = scatter_sums(me, part, landing[:n], SUM_COLORS, sum_send.at[0], sum_recv.at[0])
    own_mapped = in_plane(total[...])
    own_trials = plane[0:G, :]
    sums = me.own(mapped)
    sums[0:G, :] = own_mapped
    sums[G : G + 1, :] = column(fold(own_trials * own_trials))
    sums[G + 1 : G + 2, :] = column(fold(own_trials * own_mapped))
    sums[G + 2 : G + 3, :] = column(fold(own_mapped * own_mapped))
    sums[G + 3 : G + SUMS, :] = jnp.zeros((SUMS - 3, L), F32)
    sends += gather(me, mapped, SECOND_COLORS, second_send, second_recv)

    all_sums = jnp.zeros((SUMS, L), F32)
    for x in range(4):
        for z in range(4):
            for y in range(4):
                all_sums = all_sums + mapped[x, z, y, G : G + SUMS, :]
    squares = halves(all_sums[0:1])
    center = halves(all_sums[1:2]) / squares
    spread = jnp.sqrt(halves(all_sums[2:3]) / squares)
    unspread = 1.0 / spread

    def first_lines(y):
        t = full_rows[pl.ds(y, G, stride=G + EXTRA), :]
        m = mapped_rows[pl.ds(y, G, stride=G + SUMS), :]
        return (m - center * t) * unspread

    for copy in part_sends:
        copy.wait_send()
    respond(fields, dens, pot, shifts, kx_parts, part, first_lines)
    part_sends = scatter_sums(me, part, landing[n:], SUM_COLORS, sum_send.at[1], sum_recv.at[1])
    own_first = (own_mapped - center * own_trials) * unspread
    second = 2.0 * (in_plane(total[...]) - center * own_first) * unspread - own_trials

    other[0] = second
    swap_copy = remote(other.at[0], other.at[1], pair_send.at[1], pair_recv.at[1], me.partner())
    swap_copy.wait_recv()
    theirs = other[1]
    is_first = me.trial == 0
    a = jnp.where(is_first, second, theirs)
    b = jnp.where(is_first, theirs, second)
    turned_a = swap(a)
    turned_b = swap(b)
    for k, product in enumerate((a * a, a * turned_a, b * b, b * turned_b, a * b, a * turned_b)):
        small[0, 0, k : k + 1] = column(fold(product))
    small[0, 0, 6:8] = jnp.zeros((2, L), F32)
    sends += part_sends + [pot_copy, swap_copy]
    for phase, axis in enumerate(DIMS):
        copies = [
            remote(
                small.at[phase, 0],
                small.at[phase, by],
                small_send.at[phase, by],
                small_recv.at[phase, by],
                me.peer(axis, by),
            )
            for by in (1, 2, 3)
        ]
        for copy in copies:
            copy.wait_recv()
        small[phase + 1, 0] = (small[phase, 0] + small[phase, 1]) + (small[phase, 2] + small[phase, 3])
        sends += copies
    block = small[3, 0] * (1.0 / float(G**3))

    def entry(row, upper):
        picked = jnp.where(half, 0.0, block[row : row + 1]) if upper else jnp.where(half, block[row : row + 1], 0.0)
        return jnp.sum(picked, axis=1, keepdims=True)

    gram = {
        (0, 0): entry(0, False),
        (1, 1): entry(0, True),
        (1, 0): entry(1, False),
        (2, 2): entry(2, False),
        (3, 3): entry(2, True),
        (3, 2): entry(3, False),
        (2, 0): entry(4, False),
        (3, 1): entry(4, True),
        (3, 0): entry(5, False),
        (2, 1): entry(5, True),
    }
    lower = {}
    for j in range(4):
        rest = gram[j, j]
        for k in range(j):
            rest = rest - lower[j, k] * lower[j, k]
        lower[j, j] = jnp.sqrt(rest)
        for i in range(j + 1, 4):
            rest = gram[i, j]
            for k in range(j):
                rest = rest - lower[i, k] * lower[j, k]
            lower[i, j] = rest / lower[j, j]
    nothing = jnp.zeros((1, 1), F32)
    inverse = {(i, j): nothing for i in range(4) for j in range(4)}
    for j in range(4):
        inverse[j, j] = 1.0 / lower[j, j]
        for i in range(j + 1, 4):
            rest = nothing
            for k in range(j, i):
                rest = rest - lower[i, k] * inverse[k, j]
            inverse[i, j] = rest / lower[i, i]
    copies = (
        jnp.where(half, a, turned_a),
        jnp.where(half, turned_a, a),
        jnp.where(half, b, turned_b),
        jnp.where(half, turned_b, b),
    )
    result = None
    for u in range(4):
        here = jnp.where(is_first, inverse[0, u], inverse[2, u])
        there = jnp.where(is_first, inverse[1, u], inverse[3, u])
        term = jnp.where(half, here, there) * copies[u]
        result = term if result is None else result + term
    other[2] = result
    for k in range(G // 2):
        a = other[2, 2 * k : 2 * k + 1, :]
        b = other[2, 2 * k + 1 : 2 * k + 2, :]
        out[0, :, k * L : (k + 1) * L] = jnp.where(half, a, swap(b))
        out[1, :, k * L : (k + 1) * L] = jnp.where(half, swap(a), b)
    for copy in sends:
        copy.wait_send()


def shards(trials, orbitals, potential, coulomb, energies, frequencies, orbital_ids, freq_index):
    slots = orbitals.shape[0]
    vmem = pl.BlockSpec(memory_space=pltpu.VMEM)
    smem = pl.BlockSpec(memory_space=pltpu.SMEM)
    dma = pltpu.SemaphoreType.DMA
    field = pltpu.VMEM((slots, G + 2, GROUP, L), F32)
    near = pltpu.VMEM((slots, LINES, G, L), F32)
    stack = pltpu.VMEM((3 * G, 2 * L), BF16)
    return pl.pallas_call(
        kernel,
        out_shape=jax.ShapeDtypeStruct(trials.shape, F32),
        in_specs=[smem] * 4 + [vmem] * 4,
        out_specs=vmem,
        scratch_shapes=[
            pltpu.VMEM((4, 4, 4, G + EXTRA, L), F32),
            pltpu.VMEM((4, 4, 4, G + SUMS, L), F32),
            pltpu.VMEM((4, 4, 4, EXTRA, L), F32),
            pltpu.VMEM((slots, G, G, L), F32),
            pltpu.VMEM((G, G, L), F32),
            field,
            field,
            field,
            near,
            near,
            stack,
            stack,
            pltpu.VMEM((4, 4, 4, G, L), F32),
            pltpu.VMEM((3, G, L), F32),
            pltpu.VMEM((4, 4, 8, L), F32),
            dma((3, 23)),
            dma((3, 23)),
            dma((3, 23)),
            dma((3, 23)),
            dma((2, 3, 3, 6)),
            dma((2, 3, 3, 6)),
            dma((2,)),
            dma((2,)),
            dma((3, 4)),
            dma((3, 4)),
            *landing_shapes(SUM_COLORS),
            *landing_shapes(SUM_COLORS),
        ],
        compiler_params=pltpu.CompilerParams(
            collective_id=0, has_side_effects=True, vmem_limit_bytes=60 * 2**20
        ),
        name="filter",
    )(energies, frequencies, orbital_ids, freq_index, trials, orbitals, potential, coulomb)


def solution(mesh):
    in_specs = (
        P("trial", "orb", None),
        P("orb", None, None),
        P("orb", None),
        P(),
        P(),
        P(),
        P("orb"),
        P("orb"),
    )
    return jax.shard_map(
        shards, mesh=mesh, in_specs=in_specs, out_specs=P("trial", "orb", None), check_vma=False
    )
```

```python
import jax
import jax.numpy as jnp
from jax import lax
from jax.experimental import pallas as pl
from jax.experimental.pallas import tpu as pltpu
from jax.sharding import PartitionSpec as P

G = 64
L = 128
MESH = pl.DeviceIdType.MESH
HIGHEST = lax.Precision.HIGHEST
F32 = jnp.float32
BF16 = jnp.bfloat16
ALL = slice(None)

DIMS = ("x", "z", "y")
STRIDE = {"x": 16, "z": 4, "y": 1}

GROUP = 80
LINES = 8
MID = 1.25
EXTRA = 16
SUMS = 8

FIRST_COLORS = (
    (("y", "z", "x"), pl.ds(0, 32)),
    (("z", "x", "y"), pl.ds(32, 24)),
    (("x", "y", "z"), pl.ds(56, 24)),
)
SECOND_COLORS = (
    (("y", "z", "x"), pl.ds(0, 24)),
    (("z", "x", "y"), pl.ds(24, 24)),
    (("x", "y", "z"), pl.ds(48, 24)),
)
SUM_COLORS = (
    (("y", "z", "x"), pl.ds(0, 24)),
    (("z", "x", "y"), pl.ds(24, 24)),
    (("x", "y", "z"), pl.ds(48, 16)),
)


class Place:
    def __init__(self):
        self.orb = lax.axis_index("orb")
        self.trial = lax.axis_index("trial")
        self.at = {
            a: lax.rem(lax.div(self.orb, jnp.int32(STRIDE[a])), jnp.int32(4)) for a in DIMS
        }

    def step(self, axis, by):
        return lax.rem(self.at[axis] + jnp.int32(by % 4), jnp.int32(4))

    def peer(self, axis, by):
        return (self.orb + (self.step(axis, by) - self.at[axis]) * STRIDE[axis], self.trial)

    def partner(self):
        return (self.orb, 1 - self.trial)

    def own(self, ref):
        return ref.at[self.at["x"], self.at["z"], self.at["y"]]


def remote(src, dst, send_sem, recv_sem, device):
    copy = pltpu.make_async_remote_copy(
        src_ref=src,
        dst_ref=dst,
        send_sem=send_sem,
        recv_sem=recv_sem,
        device_id=device,
        device_id_type=MESH,
    )
    copy.start()
    return copy


def gather(me, full, colors, send_sem, recv_sem, meanwhile=None):
    sends = []
    routes = [
        Route(me, full, order, rows, send_sem.at[i], recv_sem.at[i], sends)
        for i, (order, rows) in enumerate(colors)
    ]
    for r in routes:
        r.first = [r.send(r.planes(), n, 0, by) for n, by in enumerate(WAYS)]
    for r in routes:
        wait_all(r.first)
        r.second = [r.send(r.planes(a=ALL), 3 + n, 1, by) for n, by in enumerate(WAYS)]
    for r in routes:
        r.outward(0)
    if meanwhile is not None:
        meanwhile()
    for n, group in ((1, -1), (2, 1)):
        for r in routes:
            r.second[n].wait_recv()
            r.outward(group)
    for r in routes:
        r.pass_on(0)
    for r in routes:
        r.second[0].wait_recv()
        r.last += [r.send(r.planes(a=ALL, b=2), 6 + n, 2, by) for n, by in enumerate(WAYS)]
    for group in (-1, 1):
        for r in routes:
            r.pass_on(group)
    for r in routes:
        wait_all(r.last)
    return sends


WAYS = (2, 1, -1)


def wait_all(copies):
    for copy in copies:
        copy.wait_recv()


class Route:
    def __init__(self, me, ref, order, rows, send_sem, recv_sem, sends):
        self.me, self.ref, self.order, self.rows = me, ref, order, rows
        self.send_sem, self.recv_sem, self.sends = send_sem, recv_sem, sends
        self.third = {}
        self.last = []

    def planes(self, a=0, b=0, c=0):
        me, (da, db, dc) = self.me, self.order
        spec = {db: me.step(db, b), dc: me.step(dc, c)}
        if a is ALL:
            spec[da] = ALL
        elif isinstance(a, tuple):
            spec[da] = pl.ds(2 * a[0], 2)
        else:
            spec[da] = me.step(da, a)
        return self.ref.at[spec["x"], spec["z"], spec["y"], self.rows]

    def send(self, src, k, axis, by, dst=None):
        copy = remote(
            src,
            src if dst is None else dst,
            self.send_sem.at[k],
            self.recv_sem.at[k],
            self.me.peer(self.order[axis], by),
        )
        self.sends.append(copy)
        return copy

    def slot(self, group):
        return 9 + 4 * (group % 4)

    def outward(self, group):
        k = self.slot(group)
        src = self.planes(a=ALL, b=group)
        self.third[group] = [self.send(src, k + n, 2, by) for n, by in enumerate((1, -1))]

    def pass_on(self, group):
        k = self.slot(group) + 2
        for half, by in ((0, 1), (1, -1)):
            self.third[group][half].wait_recv()
            self.last.append(self.send(self.planes(a=(half,), b=group, c=-by), k + half, 2, by))


def landing_shapes(colors):
    shapes = []
    for _, rows in colors:
        shapes.append(pltpu.VMEM((4, 3, 4, rows.size, L), F32))
        shapes.append(pltpu.VMEM((3, 4, rows.size, L), F32))
        shapes.append(pltpu.VMEM((3, rows.size, L), F32))
    return shapes


def scatter_sums(me, part, landing, colors, send_sem, recv_sem):
    sends = []
    routes = []
    for i, (order, rows) in enumerate(colors):
        r = Route(me, part, order, rows, send_sem.at[i], recv_sem.at[i], sends)
        r.on_c, r.on_b, r.on_a = landing[3 * i : 3 * i + 3]
        r.second = []
        routes.append(r)
    groups = (2, -1, 1, 0)
    for g, group in enumerate(groups):
        for r in routes:
            r.third[group] = [
                r.send(r.planes(a=ALL, b=group, c=by), 3 * g + n, 2, by, r.on_c.at[g, n])
                for n, by in enumerate(WAYS)
            ]
    for g, group in enumerate(groups):
        for r in routes:
            wait_all(r.third[group])
            mine = r.planes(a=ALL, b=group)
            mine[...] = (mine[...] + r.on_c[g, 0]) + (r.on_c[g, 1] + r.on_c[g, 2])
            if group != 0:
                r.second.append(r.send(mine, 12 + g, 1, group, r.on_b.at[g]))
    for r in routes:
        wait_all(r.second)
        mine = r.planes(a=ALL)
        mine[...] = (mine[...] + r.on_b[0]) + (r.on_b[1] + r.on_b[2])
        r.first = [r.send(r.planes(a=by), 15 + n, 0, by, r.on_a.at[n]) for n, by in enumerate(WAYS)]
    for r in routes:
        wait_all(r.first)
        mine = r.planes()
        mine[...] = (mine[...] + r.on_a[0]) + (r.on_a[1] + r.on_a[2])
    return sends


def lanes():
    return lax.broadcasted_iota(jnp.int32, (1, L), 1)


def swap(values):
    return pltpu.roll(values, G, 1)


def halves(values):
    low = lanes() < G
    first = jnp.sum(jnp.where(low, values, 0.0), axis=1, keepdims=True)
    second = jnp.sum(jnp.where(low, 0.0, values), axis=1, keepdims=True)
    return jnp.where(low, first, second)


def fold(values):
    t = [values[8 * k : 8 * k + 8] for k in range(8)]
    return ((t[0] + t[1]) + (t[2] + t[3])) + ((t[4] + t[5]) + (t[6] + t[7]))


def column(values):
    return jnp.sum(values, axis=0, keepdims=True)


def step_weights(m, shift):
    a = [m[k + 1] + shift * m[k] for k in range(5)]
    low10 = a[1] / a[0]
    low20 = a[2] / a[0]
    pivot1 = a[2] - low10 * a[1]
    some = pivot1 > 1e-6 * a[2]
    cross = a[3] - low10 * a[2]
    low21 = jnp.where(some, cross / pivot1, 0.0)
    pivot2 = a[4] - low20 * a[2] - low21 * cross
    more = some & (pivot2 > 1e-6 * a[4])
    y1 = m[1] - low10 * m[0]
    y2 = m[2] - low20 * m[0] - low21 * y1
    c2 = jnp.where(more, y2 / pivot2, 0.0)
    c1 = jnp.where(some, y1 / pivot1, 0.0) - low21 * c2
    c0 = m[0] / a[0] - low10 * c1 - low20 * c2
    return 2.0 * c0, 2.0 * c1, 2.0 * c2


def split(values):
    upper = values.astype(BF16)
    return upper, (values - upper.astype(F32)).astype(BF16)


def respond(fields, dens, pot, shifts, kx, part, trial_lines, after_begin=None):
    u0, u1, u2, near_even, near_odd, stack_even, stack_odd = fields
    slots = range(dens.shape[0])
    lines = near_even.shape[1]
    chunks = G // lines
    row = lax.broadcasted_iota(jnp.int32, (2 * L, L), 0) % L
    col = lax.broadcasted_iota(jnp.int32, (2 * L, L), 1)
    beside = (jnp.abs(row - col) == 1) & ((row < G) == (col < G))
    beside = jnp.where(beside, 1.0, 0.0).astype(BF16)

    def begin(y, _):
        v = trial_lines(y)
        for s in slots:
            u0[s, y + 1, 8:72] = v * dens[s, y]
        return 0

    lax.fori_loop(0, G, begin, 0, unroll=4)
    if after_begin is not None:
        after_begin()

    def along_z(u, chunk, near):
        for k in range(lines):
            y = chunk * lines + k
            upper, lower = split(jnp.concatenate([u[s, y + 1, 8:72] for s in slots], axis=0))
            sums = jnp.dot(jnp.concatenate([upper, lower], axis=1), beside, preferred_element_type=F32)
            for s in slots:
                near[s, k] = sums[G * s : G * s + G]

    def sweep(u, at_line, sums):
        along_z(u, 0, near_even)

        def pair(j, sums):
            for near, ahead, chunk in ((near_even, near_odd, 2 * j), (near_odd, near_even, 2 * j + 1)):
                along_z(u, lax.rem(chunk + 1, jnp.int32(chunks)), ahead)
                for k in range(lines):
                    y = chunk * lines + k
                    diagonal = pot[y]
                    sums = tuple(at_line(s, y, diagonal, near[s, k], sums[s]) for s in slots)
            return sums

        return lax.fori_loop(0, chunks // 2, pair, sums)

    def centred(u, s, y, diagonal, near):
        c = u[s, y + 1, 8:72]
        along_y = u[s, y, 8:72] + u[s, y + 2, 8:72]
        along_x = u[s, y + 1, 7:71] + u[s, y + 1, 9:73]
        return c, diagonal * c - (near + (along_y + along_x))

    zero = jnp.zeros((8, L), F32)

    def first_power(s, y, diagonal, near, a):
        c, q = centred(u0, s, y, diagonal, near)
        u1[s, y + 1, 8:72] = q
        return a[0] + fold(c * c), a[1] + fold(c * q), a[2] + fold(q * q)

    low_sums = sweep(u0, first_power, tuple((zero,) * 3 for _ in slots))

    def second_power(s, y, diagonal, near, a):
        c, q = centred(u1, s, y, diagonal, near)
        u2[s, y + 1, 8:72] = q
        return a[0] + fold(c * q), a[1] + fold(q * q)

    high_sums = sweep(u1, second_power, tuple((zero,) * 2 for _ in slots))

    def third_power(s, y, diagonal, near, a):
        c = u2[s, y + 1, 8:72]
        ahead = u2[s, y + 2, 8:72] + u2[s, y + 1, 9:73]
        return a + fold(c * (diagonal * c - (near + (ahead + ahead))))

    top_sums = sweep(u2, third_power, tuple(zero for _ in slots))

    weights = []
    for s in slots:
        moments = [halves(column(t)) for t in (*low_sums[s], *high_sums[s], top_sums[s])]
        weights.append(step_weights(moments, shifts[s]))

    rows = part.reshape(G * G, L)

    def gathered(j, stack):
        for k in range(2):
            y = 2 * j + k
            total = None
            for s in slots:
                w = [c * u[s, y + 1, 8:72] for c, u in zip(weights[s], (u0, u1, u2))]
                term = (w[0] + w[1] + w[2]) * dens[s, y]
                total = term if total is None else total + term
            upper, lower = split(-total)
            stack[0:G, k * L : k * L + L] = upper
            stack[G : 2 * G, k * L : k * L + L] = upper
            stack[2 * G : 3 * G, k * L : k * L + L] = lower

    def mixed(j, stack):
        sums = jnp.dot(kx, stack[...], preferred_element_type=F32)
        for k in range(2):
            rows[pl.ds(2 * j + k, G, stride=G), :] = sums[:, k * L : k * L + L]

    gathered(0, stack_even)

    def finish(j, _):
        for stack, ahead, y_pair in ((stack_even, stack_odd, 2 * j), (stack_odd, stack_even, 2 * j + 1)):
            gathered(lax.rem(y_pair + 1, jnp.int32(G // 2)), ahead)
            mixed(y_pair, stack)
        return 0

    lax.fori_loop(0, G // 4, finish, 0)


def kernel(
    energies,
    frequencies,
    orbital_ids,
    freq_index,
    trials,
    orbitals,
    potential,
    coulomb,
    out,
    orbital_lines,
    orbital_sem,
    full,
    mapped,
    pot_other,
    dens,
    pot,
    u0,
    u1,
    u2,
    near_even,
    near_odd,
    stack_even,
    stack_odd,
    part,
    other,
    small,
    first_send,
    first_recv,
    second_send,
    second_recv,
    sum_send,
    sum_recv,
    pair_send,
    pair_recv,
    small_send,
    small_recv,
    *landing,
):
    me = Place()
    slots = range(dens.shape[0])
    half = lanes() < G

    barrier = pltpu.get_barrier_semaphore()
    peers = [me.peer(a, by) for a in DIMS for by in (1, 2, 3)] + [me.partner()]
    for peer in peers:
        pl.semaphore_signal(barrier, inc=1, device_id=peer, device_id_type=MESH)

    orbital_copy = pltpu.make_async_copy(orbitals, orbital_lines, orbital_sem)
    orbital_copy.start()
    plane = me.own(full)
    for k in range(G // 2):
        a = trials[0, :, k * L : (k + 1) * L]
        b = trials[1, :, k * L : (k + 1) * L]
        plane[2 * k : 2 * k + 1, :] = jnp.where(half, a, swap(b))
        plane[2 * k + 1 : 2 * k + 2, :] = jnp.where(half, swap(a), b)
    for k in range(EXTRA):
        start = pl.multiple_of((me.trial * EXTRA + k) * L, L)
        plane[G + k : G + k + 1, :] = potential[:, pl.ds(start, L)]

    pl.semaphore_wait(barrier, len(peers))

    def prepare():
        def clear(y, _):
            for u in (u0, u1, u2):
                for s in slots:
                    u[s, y, 0:8] = jnp.zeros((8, L), F32)
                    u[s, y, 72:80] = jnp.zeros((8, L), F32)
            return 0

        for u in (u0, u1, u2):
            for s in slots:
                u[s, 0] = jnp.zeros((GROUP, L), F32)
                u[s, G + 1] = jnp.zeros((GROUP, L), F32)
        lax.fori_loop(1, G + 1, clear, 0)
        orbital_copy.wait()

        def spread_out(k, _):
            for s in slots:
                t = orbital_lines[s, :, pl.ds(pl.multiple_of(k * L, L), L)].astype(F32)
                turned = swap(t)
                dens[s, 2 * k] = jnp.where(half, t, turned)
                dens[s, 2 * k + 1] = jnp.where(half, turned, t)
            return 0

        lax.fori_loop(0, G // 2, spread_out, 0)

    sends = gather(me, full, FIRST_COLORS, first_send, first_recv, prepare)

    pot_lines = full.at[:, :, :, pl.ds(G, EXTRA)]
    pot_copy = remote(pot_lines, pot_other, pair_send.at[0], pair_recv.at[0], me.partner())

    full_rows = full.reshape(G * (G + EXTRA), L)
    other_rows = pot_other.reshape(G * EXTRA, L)
    mapped_rows = mapped.reshape(G * (G + SUMS), L)

    def level(j, base, t):
        turned = swap(t)
        y = 2 * (base + j)
        pot[y] = 2.0 * jnp.where(half, t, turned) - 2.0 * MID
        pot[y + 1] = 2.0 * jnp.where(half, turned, t) - 2.0 * MID

    def own_level(j, _):
        level(j, me.trial * EXTRA, full_rows[pl.ds(G + j, G, stride=G + EXTRA), :])
        return 0

    def other_level(j, _):
        level(j, (1 - me.trial) * EXTRA, other_rows[pl.ds(j, G, stride=EXTRA), :])
        return 0

    def levels():
        lax.fori_loop(0, EXTRA, own_level, 0, unroll=2)
        pot_copy.wait_recv()
        lax.fori_loop(0, EXTRA, other_level, 0, unroll=2)

    shifts = []
    for s in slots:
        level_shift = frequencies[freq_index[s]] - energies[orbital_ids[s]]
        shifts.append(2.0 * (3.0 + level_shift) + 2.0 * MID)

    kx = coulomb[0]
    kx_upper = kx.astype(BF16)
    kx_lower = (kx - kx_upper.astype(F32)).astype(BF16)
    kx_parts = jnp.concatenate([kx_upper, kx_lower, kx_upper], axis=1)
    kz = jnp.concatenate([coulomb[2], coulomb[2]], axis=1)
    kz = jnp.concatenate([kz, kz], axis=0)
    same = (lax.broadcasted_iota(jnp.int32, (L, L), 0) < G) == (lax.broadcasted_iota(jnp.int32, (L, L), 1) < G)
    kz = jnp.where(same, kz, 0.0)

    def in_plane(values):
        turned = lax.dot_general(
            values, kz, (((1,), (1,)), ((), ())), precision=HIGHEST, preferred_element_type=F32
        )
        return jnp.dot(coulomb[1], turned, precision=HIGHEST, preferred_element_type=F32)

    fields = (u0, u1, u2, near_even, near_odd, stack_even, stack_odd)
    total = me.own(part)
    respond(
        fields,
        dens,
        pot,
        shifts,
        kx_parts,
        part,
        lambda y: full_rows[pl.ds(y, G, stride=G + EXTRA), :],
        levels,
    )
    n = len(landing) // 2
    part_sends = scatter_sums(me, part, landing[:n], SUM_COLORS, sum_send.at[0], sum_recv.at[0])
    own_mapped = in_plane(total[...])
    own_trials = plane[0:G, :]
    sums = me.own(mapped)
    sums[0:G, :] = own_mapped
    sums[G : G + 1, :] = column(fold(own_trials * own_trials))
    sums[G + 1 : G + 2, :] = column(fold(own_trials * own_mapped))
    sums[G + 2 : G + 3, :] = column(fold(own_mapped * own_mapped))
    sums[G + 3 : G + SUMS, :] = jnp.zeros((SUMS - 3, L), F32)
    sends += gather(me, mapped, SECOND_COLORS, second_send, second_recv)

    all_sums = jnp.zeros((SUMS, L), F32)
    for x in range(4):
        for z in range(4):
            for y in range(4):
                all_sums = all_sums + mapped[x, z, y, G : G + SUMS, :]
    squares = halves(all_sums[0:1])
    center = halves(all_sums[1:2]) / squares
    spread = jnp.sqrt(halves(all_sums[2:3]) / squares)
    unspread = 1.0 / spread

    def first_lines(y):
        t = full_rows[pl.ds(y, G, stride=G + EXTRA), :]
        m = mapped_rows[pl.ds(y, G, stride=G + SUMS), :]
        return (m - center * t) * unspread

    for copy in part_sends:
        copy.wait_send()
    respond(fields, dens, pot, shifts, kx_parts, part, first_lines)
    part_sends = scatter_sums(me, part, landing[n:], SUM_COLORS, sum_send.at[1], sum_recv.at[1])
    own_first = (own_mapped - center * own_trials) * unspread
    second = 2.0 * (in_plane(total[...]) - center * own_first) * unspread - own_trials

    other[0] = second
    swap_copy = remote(other.at[0], other.at[1], pair_send.at[1], pair_recv.at[1], me.partner())
    swap_copy.wait_recv()
    theirs = other[1]
    is_first = me.trial == 0
    a = jnp.where(is_first, second, theirs)
    b = jnp.where(is_first, theirs, second)
    turned_a = swap(a)
    turned_b = swap(b)
    for k, product in enumerate((a * a, a * turned_a, b * b, b * turned_b, a * b, a * turned_b)):
        small[0, 0, k : k + 1] = column(fold(product))
    small[0, 0, 6:8] = jnp.zeros((2, L), F32)
    sends += part_sends + [pot_copy, swap_copy]
    for phase, axis in enumerate(DIMS):
        copies = [
            remote(
                small.at[phase, 0],
                small.at[phase, by],
                small_send.at[phase, by],
                small_recv.at[phase, by],
                me.peer(axis, by),
            )
            for by in (1, 2, 3)
        ]
        for copy in copies:
            copy.wait_recv()
        small[phase + 1, 0] = (small[phase, 0] + small[phase, 1]) + (small[phase, 2] + small[phase, 3])
        sends += copies
    block = small[3, 0] * (1.0 / float(G**3))

    def entry(row, upper):
        picked = jnp.where(half, 0.0, block[row : row + 1]) if upper else jnp.where(half, block[row : row + 1], 0.0)
        return jnp.sum(picked, axis=1, keepdims=True)

    gram = {
        (0, 0): entry(0, False),
        (1, 1): entry(0, True),
        (1, 0): entry(1, False),
        (2, 2): entry(2, False),
        (3, 3): entry(2, True),
        (3, 2): entry(3, False),
        (2, 0): entry(4, False),
        (3, 1): entry(4, True),
        (3, 0): entry(5, False),
        (2, 1): entry(5, True),
    }
    lower = {}
    for j in range(4):
        rest = gram[j, j]
        for k in range(j):
            rest = rest - lower[j, k] * lower[j, k]
        lower[j, j] = jnp.sqrt(rest)
        for i in range(j + 1, 4):
            rest = gram[i, j]
            for k in range(j):
                rest = rest - lower[i, k] * lower[j, k]
            lower[i, j] = rest / lower[j, j]
    nothing = jnp.zeros((1, 1), F32)
    inverse = {(i, j): nothing for i in range(4) for j in range(4)}
    for j in range(4):
        inverse[j, j] = 1.0 / lower[j, j]
        for i in range(j + 1, 4):
            rest = nothing
            for k in range(j, i):
                rest = rest - lower[i, k] * inverse[k, j]
            inverse[i, j] = rest / lower[i, i]
    copies = (
        jnp.where(half, a, turned_a),
        jnp.where(half, turned_a, a),
        jnp.where(half, b, turned_b),
        jnp.where(half, turned_b, b),
    )
    result = None
    for u in range(4):
        here = jnp.where(is_first, inverse[0, u], inverse[2, u])
        there = jnp.where(is_first, inverse[1, u], inverse[3, u])
        term = jnp.where(half, here, there) * copies[u]
        result = term if result is None else result + term
    other[2] = result
    for k in range(G // 2):
        a = other[2, 2 * k : 2 * k + 1, :]
        b = other[2, 2 * k + 1 : 2 * k + 2, :]
        out[0, :, k * L : (k + 1) * L] = jnp.where(half, a, swap(b))
        out[1, :, k * L : (k + 1) * L] = jnp.where(half, swap(a), b)
    for copy in sends:
        copy.wait_send()


def shards(trials, orbitals, potential, coulomb, energies, frequencies, orbital_ids, freq_index):
    slots = orbitals.shape[0]
    vmem = pl.BlockSpec(memory_space=pltpu.VMEM)
    smem = pl.BlockSpec(memory_space=pltpu.SMEM)
    dma = pltpu.SemaphoreType.DMA
    field = pltpu.VMEM((slots, G + 2, GROUP, L), F32)
    near = pltpu.VMEM((slots, LINES, G, L), F32)
    stack = pltpu.VMEM((3 * G, 2 * L), BF16)
    return pl.pallas_call(
        kernel,
        out_shape=jax.ShapeDtypeStruct(trials.shape, F32),
        in_specs=[smem] * 4 + [vmem, pl.BlockSpec(memory_space=pl.ANY), vmem, vmem],
        out_specs=vmem,
        scratch_shapes=[
            pltpu.VMEM(orbitals.shape, BF16),
            dma,
            pltpu.VMEM((4, 4, 4, G + EXTRA, L), F32),
            pltpu.VMEM((4, 4, 4, G + SUMS, L), F32),
            pltpu.VMEM((4, 4, 4, EXTRA, L), F32),
            pltpu.VMEM((slots, G, G, L), F32),
            pltpu.VMEM((G, G, L), F32),
            field,
            field,
            field,
            near,
            near,
            stack,
            stack,
            pltpu.VMEM((4, 4, 4, G, L), F32),
            pltpu.VMEM((3, G, L), F32),
            pltpu.VMEM((4, 4, 8, L), F32),
            dma((3, 25)),
            dma((3, 25)),
            dma((3, 25)),
            dma((3, 25)),
            dma((2, 3, 18)),
            dma((2, 3, 18)),
            dma((2,)),
            dma((2,)),
            dma((3, 4)),
            dma((3, 4)),
            *landing_shapes(SUM_COLORS),
            *landing_shapes(SUM_COLORS),
        ],
        compiler_params=pltpu.CompilerParams(
            collective_id=0, has_side_effects=True, vmem_limit_bytes=60 * 2**20
        ),
        name="filter",
    )(energies, frequencies, orbital_ids, freq_index, trials, orbitals, potential, coulomb)


def solution(mesh):
    in_specs = (
        P("trial", "orb", None),
        P("orb", None, None),
        P("orb", None),
        P(),
        P(),
        P(),
        P("orb"),
        P("orb"),
    )
    return jax.shard_map(
        shards, mesh=mesh, in_specs=in_specs, out_specs=P("trial", "orb", None), check_vma=False
    )
```

```python
import jax
import jax.numpy as jnp
from jax import lax
from jax.experimental import pallas as pl
from jax.experimental.pallas import tpu as pltpu
from jax.sharding import PartitionSpec as P

G = 64
L = 128
MESH = pl.DeviceIdType.MESH
HIGHEST = lax.Precision.HIGHEST
F32 = jnp.float32
BF16 = jnp.bfloat16
ALL = slice(None)

DIMS = ("x", "z", "y")
STRIDE = {"x": 16, "z": 4, "y": 1}

GROUP = 80
WIDE = 4
LINES = 8
MID = 1.25
EXTRA = 16
SUMS = 8

FIRST_COLORS = (
    (("x", "y", "z"), pl.ds(56, 24)),
    (("y", "z", "x"), pl.ds(0, 32)),
    (("z", "x", "y"), pl.ds(32, 24)),
)
SECOND_COLORS = (
    (("y", "z", "x"), pl.ds(0, 24)),
    (("z", "x", "y"), pl.ds(24, 24)),
    (("x", "y", "z"), pl.ds(48, 24)),
)
SUM_COLORS = (
    (("y", "z", "x"), pl.ds(0, 24)),
    (("z", "x", "y"), pl.ds(24, 24)),
    (("x", "y", "z"), pl.ds(48, 16)),
)


class Place:
    def __init__(self):
        self.orb = lax.axis_index("orb")
        self.trial = lax.axis_index("trial")
        self.at = {
            a: lax.rem(lax.div(self.orb, jnp.int32(STRIDE[a])), jnp.int32(4)) for a in DIMS
        }

    def step(self, axis, by):
        return lax.rem(self.at[axis] + jnp.int32(by % 4), jnp.int32(4))

    def peer(self, axis, by):
        return (self.orb + (self.step(axis, by) - self.at[axis]) * STRIDE[axis], self.trial)

    def partner(self):
        return (self.orb, 1 - self.trial)

    def own(self, ref):
        return ref.at[self.at["x"], self.at["z"], self.at["y"]]


def remote(src, dst, send_sem, recv_sem, device):
    copy = pltpu.make_async_remote_copy(
        src_ref=src,
        dst_ref=dst,
        send_sem=send_sem,
        recv_sem=recv_sem,
        device_id=device,
        device_id_type=MESH,
    )
    copy.start()
    return copy


def gather(me, full, colors, send_sem, recv_sem, meanwhile=None, done=None):
    sends = []
    routes = [
        Route(me, full, order, rows, send_sem.at[i], recv_sem.at[i], sends)
        for i, (order, rows) in enumerate(colors)
    ]
    for r in routes:
        r.first = [r.send(r.planes(), n, 0, by) for n, by in enumerate(WAYS)]
    for r in routes:
        wait_all(r.first)
        r.second = [r.send(r.planes(a=ALL), 3 + n, 1, by) for n, by in enumerate(WAYS)]
    for r in routes:
        r.outward(0)
    if meanwhile is not None:
        meanwhile()
    for n, group in ((1, -1), (2, 1)):
        for r in routes:
            r.second[n].wait_recv()
            r.outward(group)
    for r in routes:
        r.pass_on(0)
    for r in routes:
        r.second[0].wait_recv()
        r.last += [r.send(r.planes(a=ALL, b=2), 6 + n, 2, by) for n, by in enumerate(WAYS)]
    for group in (-1, 1):
        for r in routes:
            r.pass_on(group)
    for i, r in enumerate(routes):
        wait_all(r.last)
        if done is not None:
            done(i)
    return sends


WAYS = (2, 1, -1)


def wait_all(copies):
    for copy in copies:
        copy.wait_recv()


class Route:
    def __init__(self, me, ref, order, rows, send_sem, recv_sem, sends):
        self.me, self.ref, self.order, self.rows = me, ref, order, rows
        self.send_sem, self.recv_sem, self.sends = send_sem, recv_sem, sends
        self.third = {}
        self.last = []

    def planes(self, a=0, b=0, c=0):
        me, (da, db, dc) = self.me, self.order
        spec = {db: me.step(db, b), dc: me.step(dc, c)}
        if a is ALL:
            spec[da] = ALL
        elif isinstance(a, tuple):
            spec[da] = pl.ds(2 * a[0], 2)
        else:
            spec[da] = me.step(da, a)
        return self.ref.at[spec["x"], spec["z"], spec["y"], self.rows]

    def send(self, src, k, axis, by, dst=None):
        copy = remote(
            src,
            src if dst is None else dst,
            self.send_sem.at[k],
            self.recv_sem.at[k],
            self.me.peer(self.order[axis], by),
        )
        self.sends.append(copy)
        return copy

    def slot(self, group):
        return 9 + 4 * (group % 4)

    def outward(self, group):
        k = self.slot(group)
        src = self.planes(a=ALL, b=group)
        self.third[group] = [self.send(src, k + n, 2, by) for n, by in enumerate((1, -1))]

    def pass_on(self, group):
        k = self.slot(group) + 2
        for half, by in ((0, 1), (1, -1)):
            self.third[group][half].wait_recv()
            self.last.append(self.send(self.planes(a=(half,), b=group, c=-by), k + half, 2, by))


def landing_shapes(colors):
    shapes = []
    for _, rows in colors:
        shapes.append(pltpu.VMEM((4, 3, 4, rows.size, L), F32))
        shapes.append(pltpu.VMEM((3, 4, rows.size, L), F32))
        shapes.append(pltpu.VMEM((3, rows.size, L), F32))
    return shapes


GROUPS = (2, -1, 1, 0)


class Scatter:
    def __init__(self, me, part, landing, colors, send_sem, recv_sem):
        self.sends = []
        self.routes = []
        for i, (order, rows) in enumerate(colors):
            r = Route(me, part, order, rows, send_sem.at[i], recv_sem.at[i], self.sends)
            r.on_c, r.on_b, r.on_a = landing[3 * i : 3 * i + 3]
            r.second = []
            self.routes.append(r)

    def start(self, first_row):
        for r in self.routes:
            if r.rows.start == first_row:
                for g, group in enumerate(GROUPS):
                    r.third[group] = [
                        r.send(r.planes(a=ALL, b=group, c=by), 3 * g + n, 2, by, r.on_c.at[g, n])
                        for n, by in enumerate(WAYS)
                    ]

    def finish(self):
        for g, group in enumerate(GROUPS):
            for r in self.routes:
                wait_all(r.third[group])
                mine = r.planes(a=ALL, b=group)
                mine[...] = (mine[...] + r.on_c[g, 0]) + (r.on_c[g, 1] + r.on_c[g, 2])
                if group != 0:
                    r.second.append(r.send(mine, 12 + g, 1, group, r.on_b.at[g]))
        for r in self.routes:
            wait_all(r.second)
            mine = r.planes(a=ALL)
            mine[...] = (mine[...] + r.on_b[0]) + (r.on_b[1] + r.on_b[2])
            r.first = [r.send(r.planes(a=by), 15 + n, 0, by, r.on_a.at[n]) for n, by in enumerate(WAYS)]
        for r in self.routes:
            wait_all(r.first)
            mine = r.planes()
            mine[...] = (mine[...] + r.on_a[0]) + (r.on_a[1] + r.on_a[2])
        return self.sends


def lanes():
    return lax.broadcasted_iota(jnp.int32, (1, L), 1)


def swap(values):
    return pltpu.roll(values, G, 1)


def halves(values):
    low = lanes() < G
    first = jnp.sum(jnp.where(low, values, 0.0), axis=1, keepdims=True)
    second = jnp.sum(jnp.where(low, 0.0, values), axis=1, keepdims=True)
    return jnp.where(low, first, second)


def fold(values):
    t = [values[8 * k : 8 * k + 8] for k in range(8)]
    return ((t[0] + t[1]) + (t[2] + t[3])) + ((t[4] + t[5]) + (t[6] + t[7]))


def column(values):
    return jnp.sum(values, axis=0, keepdims=True)


def step_weights(m, shift):
    a = [m[k + 1] + shift * m[k] for k in range(5)]
    low10 = a[1] / a[0]
    low20 = a[2] / a[0]
    pivot1 = a[2] - low10 * a[1]
    some = pivot1 > 1e-6 * a[2]
    cross = a[3] - low10 * a[2]
    low21 = jnp.where(some, cross / pivot1, 0.0)
    pivot2 = a[4] - low20 * a[2] - low21 * cross
    more = some & (pivot2 > 1e-6 * a[4])
    y1 = m[1] - low10 * m[0]
    y2 = m[2] - low20 * m[0] - low21 * y1
    c2 = jnp.where(more, y2 / pivot2, 0.0)
    c1 = jnp.where(some, y1 / pivot1, 0.0) - low21 * c2
    c0 = m[0] / a[0] - low10 * c1 - low20 * c2
    return 2.0 * c0, 2.0 * c1, 2.0 * c2


def split(values):
    upper = values.astype(BF16)
    return upper, (values - upper.astype(F32)).astype(BF16)


def respond(fields, dens, pot, shifts, kx, part, trial_lines, after_begin=None, bands=((0, G),), after_band=None):
    u0, u1, u2, near_even, near_odd, stack_even, stack_odd = fields
    slots = range(dens.shape[0])
    lines = near_even.shape[1]
    chunks = G // lines
    row = lax.broadcasted_iota(jnp.int32, (2 * L, L), 0) % L
    col = lax.broadcasted_iota(jnp.int32, (2 * L, L), 1)
    beside = (jnp.abs(row - col) == 1) & ((row < G) == (col < G))
    beside = jnp.where(beside, 1.0, 0.0).astype(BF16)

    def begin(y, _):
        v = trial_lines(y)
        for s in slots:
            u0[s, y + 1, 8:72] = v * dens[s, y]
        return 0

    lax.fori_loop(0, G, begin, 0, unroll=4)
    if after_begin is not None:
        after_begin()

    def along_z(u, chunk, near):
        for k in range(lines):
            y = chunk * lines + k
            upper, lower = split(jnp.concatenate([u[s, y + 1, 8:72] for s in slots], axis=0))
            sums = jnp.dot(jnp.concatenate([upper, lower], axis=1), beside, preferred_element_type=F32)
            for s in slots:
                near[s, k] = sums[G * s : G * s + G]

    def sweep(u, at_line, sums):
        along_z(u, 0, near_even)

        def pair(j, sums):
            for near, ahead, chunk in ((near_even, near_odd, 2 * j), (near_odd, near_even, 2 * j + 1)):
                along_z(u, lax.rem(chunk + 1, jnp.int32(chunks)), ahead)
                for k in range(lines):
                    y = chunk * lines + k
                    diagonal = pot[y]
                    sums = tuple(at_line(s, y, diagonal, near[s, k], sums[s]) for s in slots)
            return sums

        return lax.fori_loop(0, chunks // 2, pair, sums)

    def centred(u, s, y, diagonal, near):
        c = u[s, y + 1, 8:72]
        along_y = u[s, y, 8:72] + u[s, y + 2, 8:72]
        along_x = u[s, y + 1, 7:71] + u[s, y + 1, 9:73]
        return c, diagonal * c - (near + (along_y + along_x))

    zero = jnp.zeros((8, L), F32)

    def first_power(s, y, diagonal, near, a):
        c, q = centred(u0, s, y, diagonal, near)
        u1[s, y + 1, 8:72] = q
        return a[0] + fold(c * c), a[1] + fold(c * q), a[2] + fold(q * q)

    low_sums = sweep(u0, first_power, tuple((zero,) * 3 for _ in slots))

    def second_power(s, y, diagonal, near, a):
        c, q = centred(u1, s, y, diagonal, near)
        u2[s, y + 1, 8:72] = q
        return a[0] + fold(c * q), a[1] + fold(q * q)

    high_sums = sweep(u1, second_power, tuple((zero,) * 2 for _ in slots))

    def third_power(s, y, diagonal, near, a):
        c = u2[s, y + 1, 8:72]
        ahead = u2[s, y + 2, 8:72] + u2[s, y + 1, 9:73]
        return a + fold(c * (diagonal * c - (near + (ahead + ahead))))

    top_sums = sweep(u2, third_power, tuple(zero for _ in slots))

    weights = []
    for s in slots:
        moments = [halves(column(t)) for t in (*low_sums[s], *high_sums[s], top_sums[s])]
        weights.append(step_weights(moments, shifts[s]))

    rows = part.reshape(G * G, L)
    wide = stack_even.shape[1] // L

    def gathered(j, stack):
        for k in range(wide):
            y = wide * j + k
            total = None
            for s in slots:
                w = [c * u[s, y + 1, 8:72] for c, u in zip(weights[s], (u0, u1, u2))]
                term = (w[0] + w[1] + w[2]) * dens[s, y]
                total = term if total is None else total + term
            upper, lower = split(total)
            stack[0:G, k * L : k * L + L] = upper
            stack[G : 2 * G, k * L : k * L + L] = upper
            stack[2 * G : 3 * G, k * L : k * L + L] = lower

    def mixed(j, stack):
        sums = jnp.dot(kx, stack[...], preferred_element_type=F32)
        for k in range(wide):
            rows[pl.ds(wide * j + k, G, stride=G), :] = sums[:, k * L : k * L + L]

    gathered(0, stack_even)

    def finish(j, _):
        for stack, ahead, at in ((stack_even, stack_odd, 2 * j), (stack_odd, stack_even, 2 * j + 1)):
            gathered(lax.rem(at + 1, jnp.int32(G // wide)), ahead)
            mixed(at, stack)
        return 0

    for start, stop in bands:
        lax.fori_loop(start // (2 * wide), stop // (2 * wide), finish, 0)
        if after_band is not None:
            after_band(start)


def kernel(
    energies,
    frequencies,
    orbital_ids,
    freq_index,
    trials,
    orbitals,
    potential,
    coulomb,
    out,
    orbital_lines,
    orbital_sem,
    full,
    mapped,
    pot_other,
    dens,
    pot,
    u0,
    u1,
    u2,
    near_even,
    near_odd,
    stack_even,
    stack_odd,
    part,
    other,
    small,
    first_send,
    first_recv,
    second_send,
    second_recv,
    sum_send,
    sum_recv,
    pair_send,
    pair_recv,
    small_send,
    small_recv,
    *landing,
):
    me = Place()
    slots = range(dens.shape[0])
    half = lanes() < G

    barrier = pltpu.get_barrier_semaphore()
    peers = [me.peer(a, by) for a in DIMS for by in (1, 2, 3)] + [me.partner()]
    for peer in peers:
        pl.semaphore_signal(barrier, inc=1, device_id=peer, device_id_type=MESH)

    orbital_copy = pltpu.make_async_copy(orbitals, orbital_lines, orbital_sem)
    orbital_copy.start()
    plane = me.own(full)
    for k in range(G // 2):
        a = trials[0, :, k * L : (k + 1) * L]
        b = trials[1, :, k * L : (k + 1) * L]
        plane[2 * k : 2 * k + 1, :] = jnp.where(half, a, swap(b))
        plane[2 * k + 1 : 2 * k + 2, :] = jnp.where(half, swap(a), b)
    for k in range(EXTRA):
        start = pl.multiple_of((me.trial * EXTRA + k) * L, L)
        plane[G + k : G + k + 1, :] = potential[:, pl.ds(start, L)]

    pl.semaphore_wait(barrier, len(peers))

    def prepare():
        def clear(y, _):
            for u in (u0, u1, u2):
                for s in slots:
                    u[s, y, 0:8] = jnp.zeros((8, L), F32)
                    u[s, y, 72:80] = jnp.zeros((8, L), F32)
            return 0

        for u in (u0, u1, u2):
            for s in slots:
                u[s, 0] = jnp.zeros((GROUP, L), F32)
                u[s, G + 1] = jnp.zeros((GROUP, L), F32)
        lax.fori_loop(1, G + 1, clear, 0)
        orbital_copy.wait()

        def spread_out(k, _):
            for s in slots:
                t = orbital_lines[s, :, pl.ds(pl.multiple_of(k * L, L), L)].astype(F32)
                turned = swap(t)
                dens[s, 2 * k] = jnp.where(half, t, turned)
                dens[s, 2 * k + 1] = jnp.where(half, turned, t)
            return 0

        lax.fori_loop(0, G // 2, spread_out, 0)

    full_rows = full.reshape(G * (G + EXTRA), L)
    other_rows = pot_other.reshape(G * EXTRA, L)
    mapped_rows = mapped.reshape(G * (G + SUMS), L)

    def level(j, base, t):
        turned = swap(t)
        y = 2 * (base + j)
        pot[y] = 2.0 * jnp.where(half, t, turned) - 2.0 * MID
        pot[y + 1] = 2.0 * jnp.where(half, turned, t) - 2.0 * MID

    def own_level(j, _):
        level(j, me.trial * EXTRA, full_rows[pl.ds(G + j, G, stride=G + EXTRA), :])
        return 0

    def other_level(j, _):
        level(j, (1 - me.trial) * EXTRA, other_rows[pl.ds(j, G, stride=EXTRA), :])
        return 0

    pot_copies = []

    def exchange_potential(color):
        if color == 0:
            lines = full.at[:, :, :, pl.ds(G, EXTRA)]
            pot_copies.append(remote(lines, pot_other, pair_send.at[0], pair_recv.at[0], me.partner()))
            lax.fori_loop(0, EXTRA, own_level, 0, unroll=2)

    sends = gather(me, full, FIRST_COLORS, first_send, first_recv, prepare, exchange_potential)
    (pot_copy,) = pot_copies

    def levels():
        pot_copy.wait_recv()
        lax.fori_loop(0, EXTRA, other_level, 0, unroll=2)

    shifts = []
    for s in slots:
        level_shift = frequencies[freq_index[s]] - energies[orbital_ids[s]]
        shifts.append(2.0 * (3.0 + level_shift) + 2.0 * MID)

    kx = coulomb[0]
    kx_upper = kx.astype(BF16)
    kx_lower = (kx - kx_upper.astype(F32)).astype(BF16)
    kx_parts = -jnp.concatenate([kx_upper, kx_lower, kx_upper], axis=1)
    kz = jnp.concatenate([coulomb[2], coulomb[2]], axis=1)
    kz = jnp.concatenate([kz, kz], axis=0)
    same = (lax.broadcasted_iota(jnp.int32, (L, L), 0) < G) == (lax.broadcasted_iota(jnp.int32, (L, L), 1) < G)
    kz = jnp.where(same, kz, 0.0)

    def in_plane(values):
        turned = lax.dot_general(
            values, kz, (((1,), (1,)), ((), ())), precision=HIGHEST, preferred_element_type=F32
        )
        return jnp.dot(coulomb[1], turned, precision=HIGHEST, preferred_element_type=F32)

    bands = [(rows.start, rows.start + rows.size) for _, rows in SUM_COLORS]
    fields = (u0, u1, u2, near_even, near_odd, stack_even, stack_odd)
    total = me.own(part)
    n = len(landing) // 2
    scatter = Scatter(me, part, landing[:n], SUM_COLORS, sum_send.at[0], sum_recv.at[0])
    respond(
        fields,
        dens,
        pot,
        shifts,
        kx_parts,
        part,
        lambda y: full_rows[pl.ds(y, G, stride=G + EXTRA), :],
        levels,
        bands,
        scatter.start,
    )
    part_sends = scatter.finish()
    own_mapped = in_plane(total[...])
    own_trials = plane[0:G, :]
    sums = me.own(mapped)
    sums[0:G, :] = own_mapped
    sums[G : G + 1, :] = column(fold(own_trials * own_trials))
    sums[G + 1 : G + 2, :] = column(fold(own_trials * own_mapped))
    sums[G + 2 : G + 3, :] = column(fold(own_mapped * own_mapped))
    sums[G + 3 : G + SUMS, :] = jnp.zeros((SUMS - 3, L), F32)
    sends += gather(me, mapped, SECOND_COLORS, second_send, second_recv)

    all_sums = jnp.zeros((SUMS, L), F32)
    for x in range(4):
        for z in range(4):
            for y in range(4):
                all_sums = all_sums + mapped[x, z, y, G : G + SUMS, :]
    squares = halves(all_sums[0:1])
    center = halves(all_sums[1:2]) / squares
    spread = jnp.sqrt(halves(all_sums[2:3]) / squares)
    unspread = 1.0 / spread

    def first_lines(y):
        t = full_rows[pl.ds(y, G, stride=G + EXTRA), :]
        m = mapped_rows[pl.ds(y, G, stride=G + SUMS), :]
        return (m - center * t) * unspread

    for copy in part_sends:
        copy.wait_send()
    scatter = Scatter(me, part, landing[n:], SUM_COLORS, sum_send.at[1], sum_recv.at[1])
    respond(fields, dens, pot, shifts, kx_parts, part, first_lines, None, bands, scatter.start)
    part_sends = scatter.finish()
    own_first = (own_mapped - center * own_trials) * unspread
    second = 2.0 * (in_plane(total[...]) - center * own_first) * unspread - own_trials

    other[0] = second
    swap_copy = remote(other.at[0], other.at[1], pair_send.at[1], pair_recv.at[1], me.partner())
    swap_copy.wait_recv()
    theirs = other[1]
    is_first = me.trial == 0
    a = jnp.where(is_first, second, theirs)
    b = jnp.where(is_first, theirs, second)
    turned_a = swap(a)
    turned_b = swap(b)
    for k, product in enumerate((a * a, a * turned_a, b * b, b * turned_b, a * b, a * turned_b)):
        small[0, 0, k : k + 1] = column(fold(product))
    small[0, 0, 6:8] = jnp.zeros((2, L), F32)
    sends += part_sends + [pot_copy, swap_copy]
    for phase, axis in enumerate(DIMS):
        copies = [
            remote(
                small.at[phase, 0],
                small.at[phase, by],
                small_send.at[phase, by],
                small_recv.at[phase, by],
                me.peer(axis, by),
            )
            for by in (1, 2, 3)
        ]
        for copy in copies:
            copy.wait_recv()
        small[phase + 1, 0] = (small[phase, 0] + small[phase, 1]) + (small[phase, 2] + small[phase, 3])
        sends += copies
    block = small[3, 0] * (1.0 / float(G**3))

    def entry(row, upper):
        picked = jnp.where(half, 0.0, block[row : row + 1]) if upper else jnp.where(half, block[row : row + 1], 0.0)
        return jnp.sum(picked, axis=1, keepdims=True)

    gram = {
        (0, 0): entry(0, False),
        (1, 1): entry(0, True),
        (1, 0): entry(1, False),
        (2, 2): entry(2, False),
        (3, 3): entry(2, True),
        (3, 2): entry(3, False),
        (2, 0): entry(4, False),
        (3, 1): entry(4, True),
        (3, 0): entry(5, False),
        (2, 1): entry(5, True),
    }
    lower = {}
    for j in range(4):
        rest = gram[j, j]
        for k in range(j):
            rest = rest - lower[j, k] * lower[j, k]
        lower[j, j] = jnp.sqrt(rest)
        for i in range(j + 1, 4):
            rest = gram[i, j]
            for k in range(j):
                rest = rest - lower[i, k] * lower[j, k]
            lower[i, j] = rest / lower[j, j]
    nothing = jnp.zeros((1, 1), F32)
    inverse = {(i, j): nothing for i in range(4) for j in range(4)}
    for j in range(4):
        inverse[j, j] = 1.0 / lower[j, j]
        for i in range(j + 1, 4):
            rest = nothing
            for k in range(j, i):
                rest = rest - lower[i, k] * inverse[k, j]
            inverse[i, j] = rest / lower[i, i]
    copies = (
        jnp.where(half, a, turned_a),
        jnp.where(half, turned_a, a),
        jnp.where(half, b, turned_b),
        jnp.where(half, turned_b, b),
    )
    result = None
    for u in range(4):
        here = jnp.where(is_first, inverse[0, u], inverse[2, u])
        there = jnp.where(is_first, inverse[1, u], inverse[3, u])
        term = jnp.where(half, here, there) * copies[u]
        result = term if result is None else result + term
    other[2] = result
    for k in range(G // 2):
        a = other[2, 2 * k : 2 * k + 1, :]
        b = other[2, 2 * k + 1 : 2 * k + 2, :]
        out[0, :, k * L : (k + 1) * L] = jnp.where(half, a, swap(b))
        out[1, :, k * L : (k + 1) * L] = jnp.where(half, swap(a), b)
    for copy in sends:
        copy.wait_send()


def shards(trials, orbitals, potential, coulomb, energies, frequencies, orbital_ids, freq_index):
    slots = orbitals.shape[0]
    vmem = pl.BlockSpec(memory_space=pltpu.VMEM)
    smem = pl.BlockSpec(memory_space=pltpu.SMEM)
    dma = pltpu.SemaphoreType.DMA
    field = pltpu.VMEM((slots, G + 2, GROUP, L), F32)
    near = pltpu.VMEM((slots, LINES, G, L), F32)
    stack = pltpu.VMEM((3 * G, WIDE * L), BF16)
    return pl.pallas_call(
        kernel,
        out_shape=jax.ShapeDtypeStruct(trials.shape, F32),
        in_specs=[smem] * 4 + [vmem, pl.BlockSpec(memory_space=pl.ANY), vmem, vmem],
        out_specs=vmem,
        scratch_shapes=[
            pltpu.VMEM(orbitals.shape, BF16),
            dma,
            pltpu.VMEM((4, 4, 4, G + EXTRA, L), F32),
            pltpu.VMEM((4, 4, 4, G + SUMS, L), F32),
            pltpu.VMEM((4, 4, 4, EXTRA, L), F32),
            pltpu.VMEM((slots, G, G, L), F32),
            pltpu.VMEM((G, G, L), F32),
            field,
            field,
            field,
            near,
            near,
            stack,
            stack,
            pltpu.VMEM((4, 4, 4, G, L), F32),
            pltpu.VMEM((3, G, L), F32),
            pltpu.VMEM((4, 4, 8, L), F32),
            dma((3, 25)),
            dma((3, 25)),
            dma((3, 25)),
            dma((3, 25)),
            dma((2, 3, 18)),
            dma((2, 3, 18)),
            dma((2,)),
            dma((2,)),
            dma((3, 4)),
            dma((3, 4)),
            *landing_shapes(SUM_COLORS),
            *landing_shapes(SUM_COLORS),
        ],
        compiler_params=pltpu.CompilerParams(
            collective_id=0, has_side_effects=True, vmem_limit_bytes=60 * 2**20
        ),
        name="filter",
    )(energies, frequencies, orbital_ids, freq_index, trials, orbitals, potential, coulomb)


def solution(mesh):
    in_specs = (
        P("trial", "orb", None),
        P("orb", None, None),
        P("orb", None),
        P(),
        P(),
        P(),
        P("orb"),
        P("orb"),
    )
    return jax.shard_map(
        shards, mesh=mesh, in_specs=in_specs, out_specs=P("trial", "orb", None), check_vma=False
    )
```

```python
import jax
import jax.numpy as jnp
from jax import lax
from jax.experimental import pallas as pl
from jax.experimental.pallas import tpu as pltpu
from jax.sharding import PartitionSpec as P

G = 64
L = 128
MESH = pl.DeviceIdType.MESH
HIGHEST = lax.Precision.HIGHEST
F32 = jnp.float32
BF16 = jnp.bfloat16
ALL = slice(None)

DIMS = ("x", "z", "y")
STRIDE = {"x": 16, "z": 4, "y": 1}

GROUP = 80
WIDE = 4
LINES = 8
MID = 1.25
EXTRA = 16
SUMS = 8

FIRST_COLORS = (
    (("x", "y", "z"), pl.ds(56, 24)),
    (("y", "z", "x"), pl.ds(0, 32)),
    (("z", "x", "y"), pl.ds(32, 24)),
)
SECOND_COLORS = (
    (("y", "z", "x"), pl.ds(0, 24)),
    (("z", "x", "y"), pl.ds(24, 24)),
    (("x", "y", "z"), pl.ds(48, 24)),
)
SUM_COLORS = (
    (("y", "z", "x"), pl.ds(0, 24)),
    (("z", "x", "y"), pl.ds(24, 24)),
    (("x", "y", "z"), pl.ds(48, 16)),
)


class Place:
    def __init__(self):
        self.orb = lax.axis_index("orb")
        self.trial = lax.axis_index("trial")
        self.at = {
            a: lax.rem(lax.div(self.orb, jnp.int32(STRIDE[a])), jnp.int32(4)) for a in DIMS
        }

    def step(self, axis, by):
        return lax.rem(self.at[axis] + jnp.int32(by % 4), jnp.int32(4))

    def peer(self, axis, by):
        return (self.orb + (self.step(axis, by) - self.at[axis]) * STRIDE[axis], self.trial)

    def partner(self):
        return (self.orb, 1 - self.trial)

    def own(self, ref):
        return ref.at[self.at["x"], self.at["z"], self.at["y"]]


def remote(src, dst, send_sem, recv_sem, device):
    copy = pltpu.make_async_remote_copy(
        src_ref=src,
        dst_ref=dst,
        send_sem=send_sem,
        recv_sem=recv_sem,
        device_id=device,
        device_id_type=MESH,
    )
    copy.start()
    return copy


def gather(me, full, colors, send_sem, recv_sem, meanwhile=None, done=None):
    sends = []
    routes = [
        Route(me, full, order, rows, send_sem.at[i], recv_sem.at[i], sends)
        for i, (order, rows) in enumerate(colors)
    ]
    for r in routes:
        r.first = [r.send(r.planes(), n, 0, by) for n, by in enumerate(WAYS)]
    for r in routes:
        wait_all(r.first)
        r.second = [r.send(r.planes(a=ALL), 3 + n, 1, by) for n, by in enumerate(WAYS)]
    for r in routes:
        r.outward(0)
    if meanwhile is not None:
        meanwhile()
    for n, group in ((1, -1), (2, 1)):
        for r in routes:
            r.second[n].wait_recv()
            r.outward(group)
    for r in routes:
        r.pass_on(0)
    for r in routes:
        r.second[0].wait_recv()
        r.last += [r.send(r.planes(a=ALL, b=2), 6 + n, 2, by) for n, by in enumerate(WAYS)]
    for group in (-1, 1):
        for r in routes:
            r.pass_on(group)
    for i, r in enumerate(routes):
        wait_all(r.last)
        if done is not None:
            done(i)
    return sends


WAYS = (2, 1, -1)


def wait_all(copies):
    for copy in copies:
        copy.wait_recv()


class Route:
    def __init__(self, me, ref, order, rows, send_sem, recv_sem, sends):
        self.me, self.ref, self.order, self.rows = me, ref, order, rows
        self.send_sem, self.recv_sem, self.sends = send_sem, recv_sem, sends
        self.third = {}
        self.last = []

    def planes(self, a=0, b=0, c=0):
        me, (da, db, dc) = self.me, self.order
        spec = {db: me.step(db, b), dc: me.step(dc, c)}
        if a is ALL:
            spec[da] = ALL
        elif isinstance(a, tuple):
            spec[da] = pl.ds(2 * a[0], 2)
        else:
            spec[da] = me.step(da, a)
        return self.ref.at[spec["x"], spec["z"], spec["y"], self.rows]

    def send(self, src, k, axis, by, dst=None):
        copy = remote(
            src,
            src if dst is None else dst,
            self.send_sem.at[k],
            self.recv_sem.at[k],
            self.me.peer(self.order[axis], by),
        )
        self.sends.append(copy)
        return copy

    def slot(self, group):
        return 9 + 4 * (group % 4)

    def outward(self, group):
        k = self.slot(group)
        src = self.planes(a=ALL, b=group)
        self.third[group] = [self.send(src, k + n, 2, by) for n, by in enumerate((1, -1))]

    def pass_on(self, group):
        k = self.slot(group) + 2
        for half, by in ((0, 1), (1, -1)):
            self.third[group][half].wait_recv()
            self.last.append(self.send(self.planes(a=(half,), b=group, c=-by), k + half, 2, by))


def landing_shapes(colors):
    shapes = []
    for _, rows in colors:
        shapes.append(pltpu.VMEM((4, 3, 4, rows.size, L), F32))
        shapes.append(pltpu.VMEM((3, 4, rows.size, L), F32))
        shapes.append(pltpu.VMEM((3, rows.size, L), F32))
    return shapes


GROUPS = (2, -1, 1, 0)


class Scatter:
    def __init__(self, me, part, landing, colors, send_sem, recv_sem):
        self.sends = []
        self.routes = []
        for i, (order, rows) in enumerate(colors):
            r = Route(me, part, order, rows, send_sem.at[i], recv_sem.at[i], self.sends)
            r.on_c, r.on_b, r.on_a = landing[3 * i : 3 * i + 3]
            r.second = []
            self.routes.append(r)

    def start(self, first_row):
        for r in self.routes:
            if r.rows.start == first_row:
                for g, group in enumerate(GROUPS):
                    r.third[group] = [
                        r.send(r.planes(a=ALL, b=group, c=by), 3 * g + n, 2, by, r.on_c.at[g, n])
                        for n, by in enumerate(WAYS)
                    ]

    def finish(self):
        for g, group in enumerate(GROUPS):
            for r in self.routes:
                wait_all(r.third[group])
                mine = r.planes(a=ALL, b=group)
                mine[...] = (mine[...] + r.on_c[g, 0]) + (r.on_c[g, 1] + r.on_c[g, 2])
                if group != 0:
                    r.second.append(r.send(mine, 12 + g, 1, group, r.on_b.at[g]))
        for r in self.routes:
            wait_all(r.second)
            mine = r.planes(a=ALL)
            mine[...] = (mine[...] + r.on_b[0]) + (r.on_b[1] + r.on_b[2])
            r.first = [r.send(r.planes(a=by), 15 + n, 0, by, r.on_a.at[n]) for n, by in enumerate(WAYS)]
        for r in self.routes:
            wait_all(r.first)
            mine = r.planes()
            mine[...] = (mine[...] + r.on_a[0]) + (r.on_a[1] + r.on_a[2])
        return self.sends


def lanes():
    return lax.broadcasted_iota(jnp.int32, (1, L), 1)


def swap(values):
    return pltpu.roll(values, G, 1)


def halves(values):
    low = lanes() < G
    first = jnp.sum(jnp.where(low, values, 0.0), axis=1, keepdims=True)
    second = jnp.sum(jnp.where(low, 0.0, values), axis=1, keepdims=True)
    return jnp.where(low, first, second)


def fold(values):
    t = [values[8 * k : 8 * k + 8] for k in range(8)]
    return ((t[0] + t[1]) + (t[2] + t[3])) + ((t[4] + t[5]) + (t[6] + t[7]))


def column(values):
    return jnp.sum(values, axis=0, keepdims=True)


def step_weights(m, shift):
    a = [m[k + 1] + shift * m[k] for k in range(5)]
    low10 = a[1] / a[0]
    low20 = a[2] / a[0]
    pivot1 = a[2] - low10 * a[1]
    some = pivot1 > 1e-6 * a[2]
    cross = a[3] - low10 * a[2]
    low21 = jnp.where(some, cross / pivot1, 0.0)
    pivot2 = a[4] - low20 * a[2] - low21 * cross
    more = some & (pivot2 > 1e-6 * a[4])
    y1 = m[1] - low10 * m[0]
    y2 = m[2] - low20 * m[0] - low21 * y1
    c2 = jnp.where(more, y2 / pivot2, 0.0)
    c1 = jnp.where(some, y1 / pivot1, 0.0) - low21 * c2
    c0 = m[0] / a[0] - low10 * c1 - low20 * c2
    return 2.0 * c0, 2.0 * c1, 2.0 * c2


def split(values):
    upper = values.astype(BF16)
    return upper, (values - upper.astype(F32)).astype(BF16)


def respond(fields, dens, pot, shifts, kx, part, trial_lines, after_begin=None, bands=((0, G),), after_band=None):
    u0, u1, u2, near_even, near_odd, stack_even, stack_odd = fields
    slots = range(dens.shape[0])
    lines = near_even.shape[1]
    chunks = G // lines
    row = lax.broadcasted_iota(jnp.int32, (2 * L, L), 0) % L
    col = lax.broadcasted_iota(jnp.int32, (2 * L, L), 1)
    beside = (jnp.abs(row - col) == 1) & ((row < G) == (col < G))
    beside = jnp.where(beside, 1.0, 0.0).astype(BF16)

    def begin(y, _):
        v = trial_lines(y)
        for s in slots:
            u0[s, y + 1, 8:72] = v * dens[s, y]
        return 0

    lax.fori_loop(0, G, begin, 0, unroll=4)
    if after_begin is not None:
        after_begin()

    def along_z(u, chunk, near):
        for k in range(lines):
            y = chunk * lines + k
            upper, lower = split(jnp.concatenate([u[s, y + 1, 8:72] for s in slots], axis=0))
            sums = jnp.dot(jnp.concatenate([upper, lower], axis=1), beside, preferred_element_type=F32)
            for s in slots:
                near[s, k] = sums[G * s : G * s + G]

    def sweep(u, at_line, sums):
        along_z(u, 0, near_even)

        def pair(j, sums):
            for near, ahead, chunk in ((near_even, near_odd, 2 * j), (near_odd, near_even, 2 * j + 1)):
                along_z(u, lax.rem(chunk + 1, jnp.int32(chunks)), ahead)
                for k in range(lines):
                    y = chunk * lines + k
                    diagonal = pot[y]
                    sums = tuple(at_line(s, y, diagonal, near[s, k], sums[s]) for s in slots)
            return sums

        return lax.fori_loop(0, chunks // 2, pair, sums)

    def centred(u, s, y, diagonal, near):
        c = u[s, y + 1, 8:72]
        along_y = u[s, y, 8:72] + u[s, y + 2, 8:72]
        along_x = u[s, y + 1, 7:71] + u[s, y + 1, 9:73]
        return c, diagonal * c - (near + (along_y + along_x))

    zero = jnp.zeros((8, L), F32)

    def first_power(s, y, diagonal, near, a):
        c, q = centred(u0, s, y, diagonal, near)
        u1[s, y + 1, 8:72] = q
        return a[0] + fold(c * c), a[1] + fold(c * q), a[2] + fold(q * q)

    low_sums = sweep(u0, first_power, tuple((zero,) * 3 for _ in slots))

    def second_power(s, y, diagonal, near, a):
        c, q = centred(u1, s, y, diagonal, near)
        u2[s, y + 1, 8:72] = q
        return a[0] + fold(c * q), a[1] + fold(q * q)

    high_sums = sweep(u1, second_power, tuple((zero,) * 2 for _ in slots))

    def third_power(s, y, diagonal, near, a):
        c = u2[s, y + 1, 8:72]
        ahead = u2[s, y + 2, 8:72] + u2[s, y + 1, 9:73]
        return a + fold(c * (diagonal * c - (near + (ahead + ahead))))

    top_sums = sweep(u2, third_power, tuple(zero for _ in slots))

    weights = []
    for s in slots:
        moments = [halves(column(t)) for t in (*low_sums[s], *high_sums[s], top_sums[s])]
        weights.append(step_weights(moments, shifts[s]))

    rows = part.reshape(G * G, L)
    wide = stack_even.shape[1] // L

    def gathered(j, stack):
        for k in range(wide):
            y = wide * j + k
            total = None
            for s in slots:
                w = [c * u[s, y + 1, 8:72] for c, u in zip(weights[s], (u0, u1, u2))]
                term = (w[0] + w[1] + w[2]) * dens[s, y]
                total = term if total is None else total + term
            upper, lower = split(total)
            stack[0:G, k * L : k * L + L] = upper
            stack[G : 2 * G, k * L : k * L + L] = upper
            stack[2 * G : 3 * G, k * L : k * L + L] = lower

    def mixed(j, stack):
        sums = jnp.dot(kx, stack[...], preferred_element_type=F32)
        for k in range(wide):
            rows[pl.ds(wide * j + k, G, stride=G), :] = sums[:, k * L : k * L + L]

    gathered(0, stack_even)

    def finish(j, _):
        for stack, ahead, at in ((stack_even, stack_odd, 2 * j), (stack_odd, stack_even, 2 * j + 1)):
            gathered(lax.rem(at + 1, jnp.int32(G // wide)), ahead)
            mixed(at, stack)
        return 0

    for start, stop in bands:
        lax.fori_loop(start // (2 * wide), stop // (2 * wide), finish, 0)
        if after_band is not None:
            after_band(start)


def kernel(
    energies,
    frequencies,
    orbital_ids,
    freq_index,
    trials,
    orbitals,
    potential,
    coulomb,
    out,
    orbital_lines,
    orbital_sem,
    full,
    mapped,
    pot_other,
    dens,
    pot,
    u0,
    u1,
    u2,
    near_even,
    near_odd,
    stack_even,
    stack_odd,
    part,
    other,
    small,
    first_send,
    first_recv,
    second_send,
    second_recv,
    sum_send,
    sum_recv,
    pair_send,
    pair_recv,
    small_send,
    small_recv,
    *landing,
):
    me = Place()
    slots = range(dens.shape[0])
    half = lanes() < G

    barrier = pltpu.get_barrier_semaphore()
    peers = [me.peer(a, by) for a in DIMS for by in (1, 2, 3)] + [me.partner()]
    for peer in peers:
        pl.semaphore_signal(barrier, inc=1, device_id=peer, device_id_type=MESH)

    orbital_copy = pltpu.make_async_copy(orbitals, orbital_lines, orbital_sem)
    orbital_copy.start()
    plane = me.own(full)
    for k in range(G // 2):
        a = trials[0, :, k * L : (k + 1) * L]
        b = trials[1, :, k * L : (k + 1) * L]
        plane[2 * k : 2 * k + 1, :] = jnp.where(half, a, swap(b))
        plane[2 * k + 1 : 2 * k + 2, :] = jnp.where(half, swap(a), b)
    for k in range(EXTRA):
        start = pl.multiple_of((me.trial * EXTRA + k) * L, L)
        plane[G + k : G + k + 1, :] = potential[:, pl.ds(start, L)]

    pl.semaphore_wait(barrier, len(peers))

    def prepare():
        def clear(y, _):
            for u in (u0, u1, u2):
                for s in slots:
                    u[s, y, 0:8] = jnp.zeros((8, L), F32)
                    u[s, y, 72:80] = jnp.zeros((8, L), F32)
            return 0

        for u in (u0, u1, u2):
            for s in slots:
                u[s, 0] = jnp.zeros((GROUP, L), F32)
                u[s, G + 1] = jnp.zeros((GROUP, L), F32)
        lax.fori_loop(1, G + 1, clear, 0)
        orbital_copy.wait()

        def spread_out(k, _):
            for s in slots:
                t = orbital_lines[s, :, pl.ds(pl.multiple_of(k * L, L), L)].astype(F32)
                turned = swap(t)
                dens[s, 2 * k] = jnp.where(half, t, turned)
                dens[s, 2 * k + 1] = jnp.where(half, turned, t)
            return 0

        lax.fori_loop(0, G // 2, spread_out, 0)

    full_rows = full.reshape(G * (G + EXTRA), L)
    other_rows = pot_other.reshape(G * EXTRA, L)
    mapped_rows = mapped.reshape(G * (G + SUMS), L)

    def level(j, base, t):
        turned = swap(t)
        y = 2 * (base + j)
        pot[y] = 2.0 * jnp.where(half, t, turned) - 2.0 * MID
        pot[y + 1] = 2.0 * jnp.where(half, turned, t) - 2.0 * MID

    def own_level(j, _):
        level(j, me.trial * EXTRA, full_rows[pl.ds(G + j, G, stride=G + EXTRA), :])
        return 0

    def other_level(j, _):
        level(j, (1 - me.trial) * EXTRA, other_rows[pl.ds(j, G, stride=EXTRA), :])
        return 0

    pot_copies = []

    def exchange_potential(color):
        if color == 0:
            lines = full.at[:, :, :, pl.ds(G, EXTRA)]
            pot_copies.append(remote(lines, pot_other, pair_send.at[0], pair_recv.at[0], me.partner()))
            lax.fori_loop(0, EXTRA, own_level, 0, unroll=2)

    sends = gather(me, full, FIRST_COLORS, first_send, first_recv, prepare, exchange_potential)
    (pot_copy,) = pot_copies

    def levels():
        pot_copy.wait_recv()
        lax.fori_loop(0, EXTRA, other_level, 0, unroll=2)

    shifts = []
    for s in slots:
        level_shift = frequencies[freq_index[s]] - energies[orbital_ids[s]]
        shifts.append(2.0 * (3.0 + level_shift) + 2.0 * MID)

    kx = coulomb[0]
    kx_upper = kx.astype(BF16)
    kx_lower = (kx - kx_upper.astype(F32)).astype(BF16)
    kx_parts = -jnp.concatenate([kx_upper, kx_lower, kx_upper], axis=1)
    kz = jnp.concatenate([coulomb[2], coulomb[2]], axis=1)
    kz = jnp.concatenate([kz, kz], axis=0)
    same = (lax.broadcasted_iota(jnp.int32, (L, L), 0) < G) == (lax.broadcasted_iota(jnp.int32, (L, L), 1) < G)
    kz = jnp.where(same, kz, 0.0)

    def in_plane(values):
        turned = lax.dot_general(
            values, kz, (((1,), (1,)), ((), ())), precision=HIGHEST, preferred_element_type=F32
        )
        return jnp.dot(coulomb[1], turned, precision=HIGHEST, preferred_element_type=F32)

    bands = [(rows.start, rows.start + rows.size) for _, rows in SUM_COLORS]
    fields = (u0, u1, u2, near_even, near_odd, stack_even, stack_odd)
    total = me.own(part)
    n = len(landing) // 2
    scatter = Scatter(me, part, landing[:n], SUM_COLORS, sum_send.at[0], sum_recv.at[0])
    respond(
        fields,
        dens,
        pot,
        shifts,
        kx_parts,
        part,
        lambda y: full_rows[pl.ds(y, G, stride=G + EXTRA), :],
        levels,
        bands,
        scatter.start,
    )
    part_sends = scatter.finish()
    own_mapped = in_plane(total[...])
    own_trials = plane[0:G, :]
    sums = me.own(mapped)
    sums[0:G, :] = own_mapped
    sums[G : G + 1, :] = column(fold(own_trials * own_trials))
    sums[G + 1 : G + 2, :] = column(fold(own_trials * own_mapped))
    sums[G + 2 : G + 3, :] = column(fold(own_mapped * own_mapped))
    sums[G + 3 : G + SUMS, :] = jnp.zeros((SUMS - 3, L), F32)
    sends += gather(me, mapped, SECOND_COLORS, second_send, second_recv)

    all_sums = jnp.zeros((SUMS, L), F32)
    for x in range(4):
        for z in range(4):
            for y in range(4):
                all_sums = all_sums + mapped[x, z, y, G : G + SUMS, :]
    squares = halves(all_sums[0:1])
    center = halves(all_sums[1:2]) / squares
    spread = jnp.sqrt(halves(all_sums[2:3]) / squares)
    unspread = 1.0 / spread

    def first_lines(y):
        t = full_rows[pl.ds(y, G, stride=G + EXTRA), :]
        m = mapped_rows[pl.ds(y, G, stride=G + SUMS), :]
        return (m - center * t) * unspread

    for copy in part_sends:
        copy.wait_send()
    scatter = Scatter(me, part, landing[n:], SUM_COLORS, sum_send.at[1], sum_recv.at[1])
    respond(fields, dens, pot, shifts, kx_parts, part, first_lines, None, bands, scatter.start)
    part_sends = scatter.finish()
    own_first = (own_mapped - center * own_trials) * unspread
    second = 2.0 * (in_plane(total[...]) - center * own_first) * unspread - own_trials

    other[0] = second
    swap_copy = remote(other.at[0], other.at[1], pair_send.at[1], pair_recv.at[1], me.partner())
    swap_copy.wait_recv()
    theirs = other[1]
    is_first = me.trial == 0
    a = jnp.where(is_first, second, theirs)
    b = jnp.where(is_first, theirs, second)
    turned_a = swap(a)
    turned_b = swap(b)
    place = lanes() % G
    row = jnp.zeros((1, L), F32)
    for k, product in enumerate((a * a, a * turned_a, b * b, b * turned_b, a * b, a * turned_b)):
        row = jnp.where(place == k, halves(column(fold(product))), row)
    small[me.orb] = row
    sends += part_sends + [pot_copy, swap_copy]
    everyone = small.shape[0]
    mine = small.at[me.orb]

    def tell(i, _):
        remote(
            mine, mine, small_send, small_recv, (lax.rem(me.orb + i, jnp.int32(everyone)), me.trial)
        )
        return 0

    lax.fori_loop(1, everyone, tell, 0)
    others = small.at[pl.ds(0, everyone - 1)]
    told = pltpu.make_async_remote_copy(
        src_ref=others,
        dst_ref=others,
        send_sem=small_send,
        recv_sem=small_recv,
        device_id=me.partner(),
        device_id_type=MESH,
    )
    told.wait_recv()
    sends.append(told)
    block = jnp.sum(small[...], axis=0) * (1.0 / float(G**3))

    def entry(k, upper):
        picked = jnp.where(lanes() == (k + G if upper else k), block, 0.0)
        return jnp.sum(picked, axis=1, keepdims=True)

    gram = {
        (0, 0): entry(0, False),
        (1, 1): entry(0, True),
        (1, 0): entry(1, False),
        (2, 2): entry(2, False),
        (3, 3): entry(2, True),
        (3, 2): entry(3, False),
        (2, 0): entry(4, False),
        (3, 1): entry(4, True),
        (3, 0): entry(5, False),
        (2, 1): entry(5, True),
    }
    lower = {}
    for j in range(4):
        rest = gram[j, j]
        for k in range(j):
            rest = rest - lower[j, k] * lower[j, k]
        lower[j, j] = jnp.sqrt(rest)
        for i in range(j + 1, 4):
            rest = gram[i, j]
            for k in range(j):
                rest = rest - lower[i, k] * lower[j, k]
            lower[i, j] = rest / lower[j, j]
    nothing = jnp.zeros((1, 1), F32)
    inverse = {(i, j): nothing for i in range(4) for j in range(4)}
    for j in range(4):
        inverse[j, j] = 1.0 / lower[j, j]
        for i in range(j + 1, 4):
            rest = nothing
            for k in range(j, i):
                rest = rest - lower[i, k] * inverse[k, j]
            inverse[i, j] = rest / lower[i, i]
    copies = (
        jnp.where(half, a, turned_a),
        jnp.where(half, turned_a, a),
        jnp.where(half, b, turned_b),
        jnp.where(half, turned_b, b),
    )
    result = None
    for u in range(4):
        here = jnp.where(is_first, inverse[0, u], inverse[2, u])
        there = jnp.where(is_first, inverse[1, u], inverse[3, u])
        term = jnp.where(half, here, there) * copies[u]
        result = term if result is None else result + term
    other[2] = result
    for k in range(G // 2):
        a = other[2, 2 * k : 2 * k + 1, :]
        b = other[2, 2 * k + 1 : 2 * k + 2, :]
        out[0, :, k * L : (k + 1) * L] = jnp.where(half, a, swap(b))
        out[1, :, k * L : (k + 1) * L] = jnp.where(half, swap(a), b)
    for copy in sends:
        copy.wait_send()


def shards(trials, orbitals, potential, coulomb, energies, frequencies, orbital_ids, freq_index):
    slots = orbitals.shape[0]
    vmem = pl.BlockSpec(memory_space=pltpu.VMEM)
    smem = pl.BlockSpec(memory_space=pltpu.SMEM)
    dma = pltpu.SemaphoreType.DMA
    field = pltpu.VMEM((slots, G + 2, GROUP, L), F32)
    near = pltpu.VMEM((slots, LINES, G, L), F32)
    stack = pltpu.VMEM((3 * G, WIDE * L), BF16)
    return pl.pallas_call(
        kernel,
        out_shape=jax.ShapeDtypeStruct(trials.shape, F32),
        in_specs=[smem] * 4 + [vmem, pl.BlockSpec(memory_space=pl.ANY), vmem, vmem],
        out_specs=vmem,
        scratch_shapes=[
            pltpu.VMEM(orbitals.shape, BF16),
            dma,
            pltpu.VMEM((4, 4, 4, G + EXTRA, L), F32),
            pltpu.VMEM((4, 4, 4, G + SUMS, L), F32),
            pltpu.VMEM((4, 4, 4, EXTRA, L), F32),
            pltpu.VMEM((slots, G, G, L), F32),
            pltpu.VMEM((G, G, L), F32),
            field,
            field,
            field,
            near,
            near,
            stack,
            stack,
            pltpu.VMEM((4, 4, 4, G, L), F32),
            pltpu.VMEM((3, G, L), F32),
            pltpu.VMEM((G, 1, L), F32),
            dma((3, 25)),
            dma((3, 25)),
            dma((3, 25)),
            dma((3, 25)),
            dma((2, 3, 18)),
            dma((2, 3, 18)),
            dma((2,)),
            dma((2,)),
            dma,
            dma,
            *landing_shapes(SUM_COLORS),
            *landing_shapes(SUM_COLORS),
        ],
        compiler_params=pltpu.CompilerParams(
            collective_id=0, has_side_effects=True, vmem_limit_bytes=60 * 2**20
        ),
        name="filter",
    )(energies, frequencies, orbital_ids, freq_index, trials, orbitals, potential, coulomb)


def solution(mesh):
    in_specs = (
        P("trial", "orb", None),
        P("orb", None, None),
        P("orb", None),
        P(),
        P(),
        P(),
        P("orb"),
        P("orb"),
    )
    return jax.shard_map(
        shards, mesh=mesh, in_specs=in_specs, out_specs=P("trial", "orb", None), check_vma=False
    )
```

```python
import jax
import jax.numpy as jnp
from jax import lax
from jax.experimental import pallas as pl
from jax.experimental.pallas import tpu as pltpu
from jax.sharding import PartitionSpec as P

G = 64
L = 128
MESH = pl.DeviceIdType.MESH
HIGHEST = lax.Precision.HIGHEST
F32 = jnp.float32
BF16 = jnp.bfloat16
ALL = slice(None)

DIMS = ("x", "z", "y")
STRIDE = {"x": 16, "z": 4, "y": 1}

GROUP = 80
WIDE = 4
LINES = 8
MID = 1.25
EXTRA = 16
SUMS = 8

FIRST_COLORS = (
    (("x", "y", "z"), pl.ds(56, 24)),
    (("y", "z", "x"), pl.ds(0, 32)),
    (("z", "x", "y"), pl.ds(32, 24)),
)
SECOND_COLORS = (
    (("y", "z", "x"), pl.ds(0, 24)),
    (("z", "x", "y"), pl.ds(24, 24)),
    (("x", "y", "z"), pl.ds(48, 24)),
)
SUM_COLORS = (
    (("y", "z", "x"), pl.ds(0, 24)),
    (("z", "x", "y"), pl.ds(24, 24)),
    (("x", "y", "z"), pl.ds(48, 16)),
)


class Place:
    def __init__(self):
        self.orb = lax.axis_index("orb")
        self.trial = lax.axis_index("trial")
        self.at = {
            a: lax.rem(lax.div(self.orb, jnp.int32(STRIDE[a])), jnp.int32(4)) for a in DIMS
        }

    def step(self, axis, by):
        return lax.rem(self.at[axis] + jnp.int32(by % 4), jnp.int32(4))

    def peer(self, axis, by):
        return (self.orb + (self.step(axis, by) - self.at[axis]) * STRIDE[axis], self.trial)

    def partner(self):
        return (self.orb, 1 - self.trial)

    def own(self, ref):
        return ref.at[self.at["x"], self.at["z"], self.at["y"]]


def remote(src, dst, send_sem, recv_sem, device):
    copy = pltpu.make_async_remote_copy(
        src_ref=src,
        dst_ref=dst,
        send_sem=send_sem,
        recv_sem=recv_sem,
        device_id=device,
        device_id_type=MESH,
    )
    copy.start()
    return copy


def gather(me, full, colors, send_sem, recv_sem, meanwhile=None, done=None):
    sends = []
    routes = [
        Route(me, full, order, rows, send_sem.at[i], recv_sem.at[i], sends)
        for i, (order, rows) in enumerate(colors)
    ]
    for r in routes:
        r.first = [r.send(r.planes(), n, 0, by) for n, by in enumerate(WAYS)]
    for r in routes:
        wait_all(r.first)
        r.second = [r.send(r.planes(a=ALL), 3 + n, 1, by) for n, by in enumerate(WAYS)]
    for r in routes:
        r.outward(0)
    if meanwhile is not None:
        meanwhile()
    for n, group in ((1, -1), (2, 1)):
        for r in routes:
            r.second[n].wait_recv()
            r.outward(group)
    for r in routes:
        r.pass_on(0)
    for r in routes:
        r.second[0].wait_recv()
        r.last += [r.send(r.planes(a=ALL, b=2), 6 + n, 2, by) for n, by in enumerate(WAYS)]
    for group in (-1, 1):
        for r in routes:
            r.pass_on(group)
    for i, r in enumerate(routes):
        wait_all(r.last)
        if done is not None:
            done(i)
    return sends


WAYS = (2, 1, -1)


def wait_all(copies):
    for copy in copies:
        copy.wait_recv()


class Route:
    def __init__(self, me, ref, order, rows, send_sem, recv_sem, sends):
        self.me, self.ref, self.order, self.rows = me, ref, order, rows
        self.send_sem, self.recv_sem, self.sends = send_sem, recv_sem, sends
        self.third = {}
        self.last = []

    def planes(self, a=0, b=0, c=0):
        me, (da, db, dc) = self.me, self.order
        spec = {db: me.step(db, b), dc: me.step(dc, c)}
        if a is ALL:
            spec[da] = ALL
        elif isinstance(a, tuple):
            spec[da] = pl.ds(2 * a[0], 2)
        else:
            spec[da] = me.step(da, a)
        return self.ref.at[spec["x"], spec["z"], spec["y"], self.rows]

    def send(self, src, k, axis, by, dst=None):
        copy = remote(
            src,
            src if dst is None else dst,
            self.send_sem.at[k],
            self.recv_sem.at[k],
            self.me.peer(self.order[axis], by),
        )
        self.sends.append(copy)
        return copy

    def slot(self, group):
        return 9 + 4 * (group % 4)

    def outward(self, group):
        k = self.slot(group)
        src = self.planes(a=ALL, b=group)
        self.third[group] = [self.send(src, k + n, 2, by) for n, by in enumerate((1, -1))]

    def pass_on(self, group):
        k = self.slot(group) + 2
        for half, by in ((0, 1), (1, -1)):
            self.third[group][half].wait_recv()
            self.last.append(self.send(self.planes(a=(half,), b=group, c=-by), k + half, 2, by))


def landing_shapes(colors):
    shapes = []
    for _, rows in colors:
        shapes.append(pltpu.VMEM((4, 3, 4, rows.size, L), F32))
        shapes.append(pltpu.VMEM((3, 4, rows.size, L), F32))
        shapes.append(pltpu.VMEM((3, rows.size, L), F32))
    return shapes


GROUPS = (2, -1, 1, 0)


class Scatter:
    def __init__(self, me, part, landing, colors, send_sem, recv_sem):
        self.sends = []
        self.routes = []
        for i, (order, rows) in enumerate(colors):
            r = Route(me, part, order, rows, send_sem.at[i], recv_sem.at[i], self.sends)
            r.on_c, r.on_b, r.on_a = landing[3 * i : 3 * i + 3]
            r.second = []
            self.routes.append(r)

    def start(self, first_row):
        for r in self.routes:
            if r.rows.start == first_row:
                for g, group in enumerate(GROUPS):
                    r.third[group] = [
                        r.send(r.planes(a=ALL, b=group, c=by), 3 * g + n, 2, by, r.on_c.at[g, n])
                        for n, by in enumerate(WAYS)
                    ]

    def finish(self):
        for g, group in enumerate(GROUPS):
            for r in self.routes:
                wait_all(r.third[group])
                mine = r.planes(a=ALL, b=group)
                mine[...] = (mine[...] + r.on_c[g, 0]) + (r.on_c[g, 1] + r.on_c[g, 2])
                if group != 0:
                    r.second.append(r.send(mine, 12 + g, 1, group, r.on_b.at[g]))
        for r in self.routes:
            wait_all(r.second)
            mine = r.planes(a=ALL)
            mine[...] = (mine[...] + r.on_b[0]) + (r.on_b[1] + r.on_b[2])
            r.first = [r.send(r.planes(a=by), 15 + n, 0, by, r.on_a.at[n]) for n, by in enumerate(WAYS)]
        for r in self.routes:
            wait_all(r.first)
            mine = r.planes()
            mine[...] = (mine[...] + r.on_a[0]) + (r.on_a[1] + r.on_a[2])
        return self.sends


def lanes():
    return lax.broadcasted_iota(jnp.int32, (1, L), 1)


def swap(values):
    return pltpu.roll(values, G, 1)


def halves(values):
    low = lanes() < G
    first = jnp.sum(jnp.where(low, values, 0.0), axis=1, keepdims=True)
    second = jnp.sum(jnp.where(low, 0.0, values), axis=1, keepdims=True)
    return jnp.where(low, first, second)


def fold(values):
    t = [values[8 * k : 8 * k + 8] for k in range(8)]
    return ((t[0] + t[1]) + (t[2] + t[3])) + ((t[4] + t[5]) + (t[6] + t[7]))


def column(values):
    return jnp.sum(values, axis=0, keepdims=True)


def step_weights(m, shift):
    a = [m[k + 1] + shift * m[k] for k in range(5)]
    low10 = a[1] / a[0]
    low20 = a[2] / a[0]
    pivot1 = a[2] - low10 * a[1]
    some = pivot1 > 1e-6 * a[2]
    cross = a[3] - low10 * a[2]
    low21 = jnp.where(some, cross / pivot1, 0.0)
    pivot2 = a[4] - low20 * a[2] - low21 * cross
    more = some & (pivot2 > 1e-6 * a[4])
    y1 = m[1] - low10 * m[0]
    y2 = m[2] - low20 * m[0] - low21 * y1
    c2 = jnp.where(more, y2 / pivot2, 0.0)
    c1 = jnp.where(some, y1 / pivot1, 0.0) - low21 * c2
    c0 = m[0] / a[0] - low10 * c1 - low20 * c2
    return 2.0 * c0, 2.0 * c1, 2.0 * c2


def split(values):
    upper = values.astype(BF16)
    return upper, (values - upper.astype(F32)).astype(BF16)


def respond(fields, dens, pot, shifts, kx, part, trial_lines, after_begin=None, bands=((0, G),), after_band=None):
    u0, u1, u2, near_even, near_odd, stack_even, stack_odd = fields
    slots = range(dens.shape[0])
    lines = near_even.shape[1]
    chunks = G // lines
    row = lax.broadcasted_iota(jnp.int32, (2 * L, L), 0) % L
    col = lax.broadcasted_iota(jnp.int32, (2 * L, L), 1)
    beside = (jnp.abs(row - col) == 1) & ((row < G) == (col < G))
    beside = jnp.where(beside, 1.0, 0.0).astype(BF16)

    def begin(y, _):
        v = trial_lines(y)
        for s in slots:
            u0[s, y + 1, 8:72] = v * dens[s, y]
        return 0

    lax.fori_loop(0, G, begin, 0, unroll=4)
    if after_begin is not None:
        after_begin()

    def along_z(u, chunk, near):
        for k in range(lines):
            y = chunk * lines + k
            upper, lower = split(jnp.concatenate([u[s, y + 1, 8:72] for s in slots], axis=0))
            sums = jnp.dot(jnp.concatenate([upper, lower], axis=1), beside, preferred_element_type=F32)
            for s in slots:
                near[s, k] = sums[G * s : G * s + G]

    def sweep(u, at_line, sums):
        along_z(u, 0, near_even)

        def pair(j, sums):
            for near, ahead, chunk in ((near_even, near_odd, 2 * j), (near_odd, near_even, 2 * j + 1)):
                along_z(u, lax.rem(chunk + 1, jnp.int32(chunks)), ahead)
                for k in range(lines):
                    y = chunk * lines + k
                    diagonal = pot[y]
                    sums = tuple(at_line(s, y, diagonal, near[s, k], sums[s]) for s in slots)
            return sums

        return lax.fori_loop(0, chunks // 2, pair, sums)

    def centred(u, s, y, diagonal, near):
        c = u[s, y + 1, 8:72]
        along_y = u[s, y, 8:72] + u[s, y + 2, 8:72]
        along_x = u[s, y + 1, 7:71] + u[s, y + 1, 9:73]
        return c, diagonal * c - (near + (along_y + along_x))

    zero = jnp.zeros((8, L), F32)

    def first_power(s, y, diagonal, near, a):
        c, q = centred(u0, s, y, diagonal, near)
        u1[s, y + 1, 8:72] = q
        return a[0] + fold(c * c), a[1] + fold(c * q), a[2] + fold(q * q)

    low_sums = sweep(u0, first_power, tuple((zero,) * 3 for _ in slots))

    def second_power(s, y, diagonal, near, a):
        c, q = centred(u1, s, y, diagonal, near)
        u2[s, y + 1, 8:72] = q
        return a[0] + fold(c * q), a[1] + fold(q * q)

    high_sums = sweep(u1, second_power, tuple((zero,) * 2 for _ in slots))

    def third_power(s, y, diagonal, near, a):
        c = u2[s, y + 1, 8:72]
        ahead = u2[s, y + 2, 8:72] + u2[s, y + 1, 9:73]
        return a + fold(c * (diagonal * c - (near + (ahead + ahead))))

    top_sums = sweep(u2, third_power, tuple(zero for _ in slots))

    weights = []
    for s in slots:
        moments = [halves(column(t)) for t in (*low_sums[s], *high_sums[s], top_sums[s])]
        weights.append(step_weights(moments, shifts[s]))

    rows = part.reshape(G * G, L)
    wide = stack_even.shape[1] // L

    def gathered(j, stack):
        for k in range(wide):
            y = wide * j + k
            total = None
            for s in slots:
                w = [c * u[s, y + 1, 8:72] for c, u in zip(weights[s], (u0, u1, u2))]
                term = (w[0] + w[1] + w[2]) * dens[s, y]
                total = term if total is None else total + term
            upper, lower = split(total)
            stack[0:G, k * L : k * L + L] = upper
            stack[G : 2 * G, k * L : k * L + L] = upper
            stack[2 * G : 3 * G, k * L : k * L + L] = lower

    def mixed(j, stack):
        sums = jnp.dot(kx, stack[...], preferred_element_type=F32)
        for k in range(wide):
            rows[pl.ds(wide * j + k, G, stride=G), :] = sums[:, k * L : k * L + L]

    gathered(0, stack_even)

    def finish(j, _):
        for stack, ahead, at in ((stack_even, stack_odd, 2 * j), (stack_odd, stack_even, 2 * j + 1)):
            gathered(lax.rem(at + 1, jnp.int32(G // wide)), ahead)
            mixed(at, stack)
        return 0

    for start, stop in bands:
        lax.fori_loop(start // (2 * wide), stop // (2 * wide), finish, 0)
        if after_band is not None:
            after_band(start)


def kernel(
    energies_in,
    frequencies_in,
    orbital_ids_in,
    freq_index_in,
    trials_in,
    orbitals,
    potential_in,
    coulomb_in,
    out,
    energies,
    frequencies,
    orbital_ids,
    freq_index,
    trials,
    potential,
    coulomb,
    input_sem,
    orbital_lines,
    orbital_sem,
    full,
    mapped,
    pot_other,
    dens,
    pot,
    u0,
    u1,
    u2,
    near_even,
    near_odd,
    stack_even,
    stack_odd,
    part,
    other,
    small,
    first_send,
    first_recv,
    second_send,
    second_recv,
    sum_send,
    sum_recv,
    pair_send,
    pair_recv,
    small_send,
    small_recv,
    *landing,
):
    me = Place()
    slots = range(dens.shape[0])
    half = lanes() < G

    inputs = [
        pltpu.make_async_copy(src, dst, input_sem.at[i])
        for i, (src, dst) in enumerate(
            (
                (trials_in, trials),
                (potential_in, potential),
                (coulomb_in, coulomb),
                (energies_in, energies),
                (frequencies_in, frequencies),
                (orbital_ids_in, orbital_ids),
                (freq_index_in, freq_index),
            )
        )
    ]
    for copy in inputs:
        copy.start()
    barrier = pltpu.get_barrier_semaphore()
    peers = [me.peer(a, by) for a in DIMS for by in (1, 2, 3)] + [me.partner()]
    for peer in peers:
        pl.semaphore_signal(barrier, inc=1, device_id=peer, device_id_type=MESH)

    orbital_copy = pltpu.make_async_copy(orbitals, orbital_lines, orbital_sem)
    orbital_copy.start()
    plane = me.own(full)
    for copy in inputs[:2]:
        copy.wait()
    for k in range(G // 2):
        a = trials[0, :, k * L : (k + 1) * L]
        b = trials[1, :, k * L : (k + 1) * L]
        plane[2 * k : 2 * k + 1, :] = jnp.where(half, a, swap(b))
        plane[2 * k + 1 : 2 * k + 2, :] = jnp.where(half, swap(a), b)
    for k in range(EXTRA):
        start = pl.multiple_of((me.trial * EXTRA + k) * L, L)
        plane[G + k : G + k + 1, :] = potential[:, pl.ds(start, L)]

    pl.semaphore_wait(barrier, len(peers))

    def prepare():
        def clear(y, _):
            for u in (u0, u1, u2):
                for s in slots:
                    u[s, y, 0:8] = jnp.zeros((8, L), F32)
                    u[s, y, 72:80] = jnp.zeros((8, L), F32)
            return 0

        for u in (u0, u1, u2):
            for s in slots:
                u[s, 0] = jnp.zeros((GROUP, L), F32)
                u[s, G + 1] = jnp.zeros((GROUP, L), F32)
        lax.fori_loop(1, G + 1, clear, 0)
        orbital_copy.wait()
        for copy in inputs[2:]:
            copy.wait()

        def spread_out(k, _):
            for s in slots:
                t = orbital_lines[s, :, pl.ds(pl.multiple_of(k * L, L), L)].astype(F32)
                turned = swap(t)
                dens[s, 2 * k] = jnp.where(half, t, turned)
                dens[s, 2 * k + 1] = jnp.where(half, turned, t)
            return 0

        lax.fori_loop(0, G // 2, spread_out, 0)

    full_rows = full.reshape(G * (G + EXTRA), L)
    other_rows = pot_other.reshape(G * EXTRA, L)
    mapped_rows = mapped.reshape(G * (G + SUMS), L)

    def level(j, base, t):
        turned = swap(t)
        y = 2 * (base + j)
        pot[y] = 2.0 * jnp.where(half, t, turned) - 2.0 * MID
        pot[y + 1] = 2.0 * jnp.where(half, turned, t) - 2.0 * MID

    def own_level(j, _):
        level(j, me.trial * EXTRA, full_rows[pl.ds(G + j, G, stride=G + EXTRA), :])
        return 0

    def other_level(j, _):
        level(j, (1 - me.trial) * EXTRA, other_rows[pl.ds(j, G, stride=EXTRA), :])
        return 0

    pot_copies = []

    def exchange_potential(color):
        if color == 0:
            lines = full.at[:, :, :, pl.ds(G, EXTRA)]
            pot_copies.append(remote(lines, pot_other, pair_send.at[0], pair_recv.at[0], me.partner()))
            lax.fori_loop(0, EXTRA, own_level, 0, unroll=2)

    sends = gather(me, full, FIRST_COLORS, first_send, first_recv, prepare, exchange_potential)
    (pot_copy,) = pot_copies

    def levels():
        pot_copy.wait_recv()
        lax.fori_loop(0, EXTRA, other_level, 0, unroll=2)

    shifts = []
    for s in slots:
        level_shift = frequencies[freq_index[s]] - energies[orbital_ids[s]]
        shifts.append(2.0 * (3.0 + level_shift) + 2.0 * MID)

    kx = coulomb[0]
    kx_upper = kx.astype(BF16)
    kx_lower = (kx - kx_upper.astype(F32)).astype(BF16)
    kx_parts = -jnp.concatenate([kx_upper, kx_lower, kx_upper], axis=1)
    kz = jnp.concatenate([coulomb[2], coulomb[2]], axis=1)
    kz = jnp.concatenate([kz, kz], axis=0)
    same = (lax.broadcasted_iota(jnp.int32, (L, L), 0) < G) == (lax.broadcasted_iota(jnp.int32, (L, L), 1) < G)
    kz = jnp.where(same, kz, 0.0)

    def in_plane(values):
        turned = lax.dot_general(
            values, kz, (((1,), (1,)), ((), ())), precision=HIGHEST, preferred_element_type=F32
        )
        return jnp.dot(coulomb[1], turned, precision=HIGHEST, preferred_element_type=F32)

    bands = [(rows.start, rows.start + rows.size) for _, rows in SUM_COLORS]
    fields = (u0, u1, u2, near_even, near_odd, stack_even, stack_odd)
    total = me.own(part)
    n = len(landing) // 2
    scatter = Scatter(me, part, landing[:n], SUM_COLORS, sum_send.at[0], sum_recv.at[0])
    respond(
        fields,
        dens,
        pot,
        shifts,
        kx_parts,
        part,
        lambda y: full_rows[pl.ds(y, G, stride=G + EXTRA), :],
        levels,
        bands,
        scatter.start,
    )
    part_sends = scatter.finish()
    own_mapped = in_plane(total[...])
    own_trials = plane[0:G, :]
    sums = me.own(mapped)
    sums[0:G, :] = own_mapped
    sums[G : G + 1, :] = column(fold(own_trials * own_trials))
    sums[G + 1 : G + 2, :] = column(fold(own_trials * own_mapped))
    sums[G + 2 : G + 3, :] = column(fold(own_mapped * own_mapped))
    sums[G + 3 : G + SUMS, :] = jnp.zeros((SUMS - 3, L), F32)
    sends += gather(me, mapped, SECOND_COLORS, second_send, second_recv)

    all_sums = jnp.zeros((SUMS, L), F32)
    for x in range(4):
        for z in range(4):
            for y in range(4):
                all_sums = all_sums + mapped[x, z, y, G : G + SUMS, :]
    squares = halves(all_sums[0:1])
    center = halves(all_sums[1:2]) / squares
    spread = jnp.sqrt(halves(all_sums[2:3]) / squares)
    unspread = 1.0 / spread

    def first_lines(y):
        t = full_rows[pl.ds(y, G, stride=G + EXTRA), :]
        m = mapped_rows[pl.ds(y, G, stride=G + SUMS), :]
        return (m - center * t) * unspread

    for copy in part_sends:
        copy.wait_send()
    scatter = Scatter(me, part, landing[n:], SUM_COLORS, sum_send.at[1], sum_recv.at[1])
    respond(fields, dens, pot, shifts, kx_parts, part, first_lines, None, bands, scatter.start)
    part_sends = scatter.finish()
    own_first = (own_mapped - center * own_trials) * unspread
    second = 2.0 * (in_plane(total[...]) - center * own_first) * unspread - own_trials

    other[0] = second
    swap_copy = remote(other.at[0], other.at[1], pair_send.at[1], pair_recv.at[1], me.partner())
    swap_copy.wait_recv()
    theirs = other[1]
    is_first = me.trial == 0
    a = jnp.where(is_first, second, theirs)
    b = jnp.where(is_first, theirs, second)
    turned_a = swap(a)
    turned_b = swap(b)
    place = lanes() % G
    row = jnp.zeros((1, L), F32)
    for k, product in enumerate((a * a, a * turned_a, b * b, b * turned_b, a * b, a * turned_b)):
        row = jnp.where(place == k, halves(column(fold(product))), row)
    small[me.orb] = row
    sends += part_sends + [pot_copy, swap_copy]
    everyone = small.shape[0]
    mine = small.at[me.orb]

    def tell(i, _):
        remote(
            mine, mine, small_send, small_recv, (lax.rem(me.orb + i, jnp.int32(everyone)), me.trial)
        )
        return 0

    lax.fori_loop(1, everyone, tell, 0)
    others = small.at[pl.ds(0, everyone - 1)]
    told = pltpu.make_async_remote_copy(
        src_ref=others,
        dst_ref=others,
        send_sem=small_send,
        recv_sem=small_recv,
        device_id=me.partner(),
        device_id_type=MESH,
    )
    told.wait_recv()
    sends.append(told)
    block = jnp.sum(small[...], axis=0) * (1.0 / float(G**3))

    def entry(k, upper):
        picked = jnp.where(lanes() == (k + G if upper else k), block, 0.0)
        return jnp.sum(picked, axis=1, keepdims=True)

    gram = {
        (0, 0): entry(0, False),
        (1, 1): entry(0, True),
        (1, 0): entry(1, False),
        (2, 2): entry(2, False),
        (3, 3): entry(2, True),
        (3, 2): entry(3, False),
        (2, 0): entry(4, False),
        (3, 1): entry(4, True),
        (3, 0): entry(5, False),
        (2, 1): entry(5, True),
    }
    lower = {}
    for j in range(4):
        rest = gram[j, j]
        for k in range(j):
            rest = rest - lower[j, k] * lower[j, k]
        lower[j, j] = jnp.sqrt(rest)
        for i in range(j + 1, 4):
            rest = gram[i, j]
            for k in range(j):
                rest = rest - lower[i, k] * lower[j, k]
            lower[i, j] = rest / lower[j, j]
    nothing = jnp.zeros((1, 1), F32)
    inverse = {(i, j): nothing for i in range(4) for j in range(4)}
    for j in range(4):
        inverse[j, j] = 1.0 / lower[j, j]
        for i in range(j + 1, 4):
            rest = nothing
            for k in range(j, i):
                rest = rest - lower[i, k] * inverse[k, j]
            inverse[i, j] = rest / lower[i, i]
    copies = (
        jnp.where(half, a, turned_a),
        jnp.where(half, turned_a, a),
        jnp.where(half, b, turned_b),
        jnp.where(half, turned_b, b),
    )
    result = None
    for u in range(4):
        here = jnp.where(is_first, inverse[0, u], inverse[2, u])
        there = jnp.where(is_first, inverse[1, u], inverse[3, u])
        term = jnp.where(half, here, there) * copies[u]
        result = term if result is None else result + term
    other[2] = result
    for k in range(G // 2):
        a = other[2, 2 * k : 2 * k + 1, :]
        b = other[2, 2 * k + 1 : 2 * k + 2, :]
        out[0, :, k * L : (k + 1) * L] = jnp.where(half, a, swap(b))
        out[1, :, k * L : (k + 1) * L] = jnp.where(half, swap(a), b)
    for copy in sends:
        copy.wait_send()


def shards(trials, orbitals, potential, coulomb, energies, frequencies, orbital_ids, freq_index):
    slots = orbitals.shape[0]
    vmem = pl.BlockSpec(memory_space=pltpu.VMEM)
    dma = pltpu.SemaphoreType.DMA
    field = pltpu.VMEM((slots, G + 2, GROUP, L), F32)
    near = pltpu.VMEM((slots, LINES, G, L), F32)
    stack = pltpu.VMEM((3 * G, WIDE * L), BF16)
    return pl.pallas_call(
        kernel,
        out_shape=jax.ShapeDtypeStruct(trials.shape, F32),
        in_specs=[pl.BlockSpec(memory_space=pl.ANY)] * 8,
        out_specs=vmem,
        scratch_shapes=[
            *(pltpu.SMEM(a.shape, a.dtype) for a in (energies, frequencies, orbital_ids, freq_index)),
            *(pltpu.VMEM(a.shape, a.dtype) for a in (trials, potential, coulomb)),
            dma((7,)),
            pltpu.VMEM(orbitals.shape, BF16),
            dma,
            pltpu.VMEM((4, 4, 4, G + EXTRA, L), F32),
            pltpu.VMEM((4, 4, 4, G + SUMS, L), F32),
            pltpu.VMEM((4, 4, 4, EXTRA, L), F32),
            pltpu.VMEM((slots, G, G, L), F32),
            pltpu.VMEM((G, G, L), F32),
            field,
            field,
            field,
            near,
            near,
            stack,
            stack,
            pltpu.VMEM((4, 4, 4, G, L), F32),
            pltpu.VMEM((3, G, L), F32),
            pltpu.VMEM((G, 1, L), F32),
            dma((3, 25)),
            dma((3, 25)),
            dma((3, 25)),
            dma((3, 25)),
            dma((2, 3, 18)),
            dma((2, 3, 18)),
            dma((2,)),
            dma((2,)),
            dma,
            dma,
            *landing_shapes(SUM_COLORS),
            *landing_shapes(SUM_COLORS),
        ],
        compiler_params=pltpu.CompilerParams(
            collective_id=0, has_side_effects=True, vmem_limit_bytes=60 * 2**20
        ),
        name="filter",
    )(energies, frequencies, orbital_ids, freq_index, trials, orbitals, potential, coulomb)


def solution(mesh):
    in_specs = (
        P("trial", "orb", None),
        P("orb", None, None),
        P("orb", None),
        P(),
        P(),
        P(),
        P("orb"),
        P("orb"),
    )
    return jax.shard_map(
        shards, mesh=mesh, in_specs=in_specs, out_specs=P("trial", "orb", None), check_vma=False
    )
```

```python
import jax
import jax.numpy as jnp
from jax import lax
from jax.experimental import pallas as pl
from jax.experimental.pallas import tpu as pltpu
from jax.sharding import PartitionSpec as P

G = 64
L = 128
MESH = pl.DeviceIdType.MESH
HIGHEST = lax.Precision.HIGHEST
F32 = jnp.float32
BF16 = jnp.bfloat16
ALL = slice(None)

DIMS = ("x", "z", "y")
STRIDE = {"x": 16, "z": 4, "y": 1}

GROUP = 80
WIDE = 4
LINES = 8
MID = 1.25
EXTRA = 16
SUMS = 8

FIRST_COLORS = (
    (("x", "y", "z"), pl.ds(56, 24)),
    (("y", "z", "x"), pl.ds(0, 32)),
    (("z", "x", "y"), pl.ds(32, 24)),
)
SECOND_COLORS = (
    (("y", "z", "x"), pl.ds(0, 24)),
    (("z", "x", "y"), pl.ds(24, 24)),
    (("x", "y", "z"), pl.ds(48, 24)),
)
SUM_COLORS = (
    (("y", "z", "x"), pl.ds(0, 24)),
    (("z", "x", "y"), pl.ds(24, 24)),
    (("x", "y", "z"), pl.ds(48, 16)),
)


class Place:
    def __init__(self):
        self.orb = lax.axis_index("orb")
        self.trial = lax.axis_index("trial")
        self.at = {
            a: lax.rem(lax.div(self.orb, jnp.int32(STRIDE[a])), jnp.int32(4)) for a in DIMS
        }

    def step(self, axis, by):
        return lax.rem(self.at[axis] + jnp.int32(by % 4), jnp.int32(4))

    def peer(self, axis, by):
        return (self.orb + (self.step(axis, by) - self.at[axis]) * STRIDE[axis], self.trial)

    def partner(self):
        return (self.orb, 1 - self.trial)

    def own(self, ref):
        return ref.at[self.at["x"], self.at["z"], self.at["y"]]


def remote(src, dst, send_sem, recv_sem, device):
    copy = pltpu.make_async_remote_copy(
        src_ref=src,
        dst_ref=dst,
        send_sem=send_sem,
        recv_sem=recv_sem,
        device_id=device,
        device_id_type=MESH,
    )
    copy.start()
    return copy


def gather(me, full, colors, send_sem, recv_sem, meanwhile=None, done=None):
    sends = []
    routes = [
        Route(me, full, order, rows, send_sem.at[i], recv_sem.at[i], sends)
        for i, (order, rows) in enumerate(colors)
    ]
    for r in routes:
        r.first = [r.send(r.planes(), n, 0, by) for n, by in enumerate(WAYS)]
    for r in routes:
        wait_all(r.first)
        r.second = [r.send(r.planes(a=ALL), 3 + n, 1, by) for n, by in enumerate(WAYS)]
    for r in routes:
        r.outward(0)
    if meanwhile is not None:
        meanwhile()
    for n, group in ((1, -1), (2, 1)):
        for r in routes:
            r.second[n].wait_recv()
            r.outward(group)
    for r in routes:
        r.pass_on(0)
    for r in routes:
        r.second[0].wait_recv()
        r.last += [r.send(r.planes(a=ALL, b=2), 6 + n, 2, by) for n, by in enumerate(WAYS)]
    for group in (-1, 1):
        for r in routes:
            r.pass_on(group)
    for i, r in enumerate(routes):
        wait_all(r.last)
        if done is not None:
            done(i)
    return sends


WAYS = (2, 1, -1)


def wait_all(copies):
    for copy in copies:
        copy.wait_recv()


class Route:
    def __init__(self, me, ref, order, rows, send_sem, recv_sem, sends):
        self.me, self.ref, self.order, self.rows = me, ref, order, rows
        self.send_sem, self.recv_sem, self.sends = send_sem, recv_sem, sends
        self.third = {}
        self.last = []

    def planes(self, a=0, b=0, c=0):
        me, (da, db, dc) = self.me, self.order
        spec = {db: me.step(db, b), dc: me.step(dc, c)}
        if a is ALL:
            spec[da] = ALL
        elif isinstance(a, tuple):
            spec[da] = pl.ds(2 * a[0], 2)
        else:
            spec[da] = me.step(da, a)
        return self.ref.at[spec["x"], spec["z"], spec["y"], self.rows]

    def send(self, src, k, axis, by, dst=None):
        copy = remote(
            src,
            src if dst is None else dst,
            self.send_sem.at[k],
            self.recv_sem.at[k],
            self.me.peer(self.order[axis], by),
        )
        self.sends.append(copy)
        return copy

    def slot(self, group):
        return 9 + 4 * (group % 4)

    def outward(self, group):
        k = self.slot(group)
        src = self.planes(a=ALL, b=group)
        self.third[group] = [self.send(src, k + n, 2, by) for n, by in enumerate((1, -1))]

    def pass_on(self, group):
        k = self.slot(group) + 2
        for half, by in ((0, 1), (1, -1)):
            self.third[group][half].wait_recv()
            self.last.append(self.send(self.planes(a=(half,), b=group, c=-by), k + half, 2, by))


def landing_shapes(colors):
    shapes = []
    for _, rows in colors:
        shapes.append(pltpu.VMEM((4, 3, 4, rows.size, L), F32))
        shapes.append(pltpu.VMEM((3, 4, rows.size, L), F32))
        shapes.append(pltpu.VMEM((3, rows.size, L), F32))
    return shapes


GROUPS = (2, -1, 1, 0)


class Scatter:
    def __init__(self, me, part, landing, colors, send_sem, recv_sem):
        self.sends = []
        self.routes = []
        for i, (order, rows) in enumerate(colors):
            r = Route(me, part, order, rows, send_sem.at[i], recv_sem.at[i], self.sends)
            r.on_c, r.on_b, r.on_a = landing[3 * i : 3 * i + 3]
            r.second = []
            self.routes.append(r)

    def start(self, first_row):
        for r in self.routes:
            if r.rows.start == first_row:
                for g, group in enumerate(GROUPS):
                    r.third[group] = [
                        r.send(r.planes(a=ALL, b=group, c=by), 3 * g + n, 2, by, r.on_c.at[g, n])
                        for n, by in enumerate(WAYS)
                    ]

    def finish(self):
        for g, group in enumerate(GROUPS):
            for r in self.routes:
                wait_all(r.third[group])
                mine = r.planes(a=ALL, b=group)
                mine[...] = (mine[...] + r.on_c[g, 0]) + (r.on_c[g, 1] + r.on_c[g, 2])
                if group != 0:
                    r.second.append(r.send(mine, 12 + g, 1, group, r.on_b.at[g]))
        for r in self.routes:
            wait_all(r.second)
            mine = r.planes(a=ALL)
            mine[...] = (mine[...] + r.on_b[0]) + (r.on_b[1] + r.on_b[2])
            r.first = [r.send(r.planes(a=by), 15 + n, 0, by, r.on_a.at[n]) for n, by in enumerate(WAYS)]
        for r in self.routes:
            wait_all(r.first)
            mine = r.planes()
            mine[...] = (mine[...] + r.on_a[0]) + (r.on_a[1] + r.on_a[2])
        return self.sends


def lanes():
    return lax.broadcasted_iota(jnp.int32, (1, L), 1)


def swap(values):
    return pltpu.roll(values, G, 1)


def halves(values):
    low = lanes() < G
    first = jnp.sum(jnp.where(low, values, 0.0), axis=1, keepdims=True)
    second = jnp.sum(jnp.where(low, 0.0, values), axis=1, keepdims=True)
    return jnp.where(low, first, second)


def fold(values):
    t = [values[8 * k : 8 * k + 8] for k in range(8)]
    return ((t[0] + t[1]) + (t[2] + t[3])) + ((t[4] + t[5]) + (t[6] + t[7]))


def column(values):
    return jnp.sum(values, axis=0, keepdims=True)


def step_weights(m, shift):
    a = [m[k + 1] + shift * m[k] for k in range(5)]
    low10 = a[1] / a[0]
    low20 = a[2] / a[0]
    pivot1 = a[2] - low10 * a[1]
    some = pivot1 > 1e-6 * a[2]
    cross = a[3] - low10 * a[2]
    low21 = jnp.where(some, cross / pivot1, 0.0)
    pivot2 = a[4] - low20 * a[2] - low21 * cross
    more = some & (pivot2 > 1e-6 * a[4])
    y1 = m[1] - low10 * m[0]
    y2 = m[2] - low20 * m[0] - low21 * y1
    c2 = jnp.where(more, y2 / pivot2, 0.0)
    c1 = jnp.where(some, y1 / pivot1, 0.0) - low21 * c2
    c0 = m[0] / a[0] - low10 * c1 - low20 * c2
    return 2.0 * c0, 2.0 * c1, 2.0 * c2


def split(values):
    upper = values.astype(BF16)
    return upper, (values - upper.astype(F32)).astype(BF16)


def respond(fields, dens, pot, shifts, kx, part, trial_lines, after_begin=None, bands=((0, G),), after_band=None):
    u0, u1, u2, near_even, near_odd, stack_even, stack_odd = fields
    slots = range(dens.shape[0])
    lines = near_even.shape[1]
    chunks = G // lines
    row = lax.broadcasted_iota(jnp.int32, (2 * L, L), 0) % L
    col = lax.broadcasted_iota(jnp.int32, (2 * L, L), 1)
    beside = (jnp.abs(row - col) == 1) & ((row < G) == (col < G))
    beside = jnp.where(beside, 1.0, 0.0).astype(BF16)

    def begin(y, _):
        v = trial_lines(y)
        for s in slots:
            u0[s, y + 1, 8:72] = v * dens[s, y]
        return 0

    lax.fori_loop(0, G, begin, 0, unroll=8)
    if after_begin is not None:
        after_begin()

    def along_z(u, chunk, near):
        for k in range(lines):
            y = chunk * lines + k
            upper, lower = split(jnp.concatenate([u[s, y + 1, 8:72] for s in slots], axis=0))
            sums = jnp.dot(jnp.concatenate([upper, lower], axis=1), beside, preferred_element_type=F32)
            for s in slots:
                near[s, k] = sums[G * s : G * s + G]

    def sweep(u, at_line, sums):
        along_z(u, 0, near_even)

        def pair(j, sums):
            for near, ahead, chunk in ((near_even, near_odd, 2 * j), (near_odd, near_even, 2 * j + 1)):
                along_z(u, lax.rem(chunk + 1, jnp.int32(chunks)), ahead)
                for k in range(lines):
                    y = chunk * lines + k
                    diagonal = pot[y]
                    sums = tuple(at_line(s, y, diagonal, near[s, k], sums[s]) for s in slots)
            return sums

        return lax.fori_loop(0, chunks // 2, pair, sums)

    def centred(u, s, y, diagonal, near):
        c = u[s, y + 1, 8:72]
        along_y = u[s, y, 8:72] + u[s, y + 2, 8:72]
        along_x = u[s, y + 1, 7:71] + u[s, y + 1, 9:73]
        return c, diagonal * c - (near + (along_y + along_x))

    zero = jnp.zeros((8, L), F32)

    def first_power(s, y, diagonal, near, a):
        c, q = centred(u0, s, y, diagonal, near)
        u1[s, y + 1, 8:72] = q
        return a[0] + fold(c * c), a[1] + fold(c * q), a[2] + fold(q * q)

    low_sums = sweep(u0, first_power, tuple((zero,) * 3 for _ in slots))

    def second_power(s, y, diagonal, near, a):
        c, q = centred(u1, s, y, diagonal, near)
        u2[s, y + 1, 8:72] = q
        return a[0] + fold(c * q), a[1] + fold(q * q)

    high_sums = sweep(u1, second_power, tuple((zero,) * 2 for _ in slots))

    def third_power(s, y, diagonal, near, a):
        c = u2[s, y + 1, 8:72]
        ahead = u2[s, y + 2, 8:72] + u2[s, y + 1, 9:73]
        return a + fold(c * (diagonal * c - (near + (ahead + ahead))))

    top_sums = sweep(u2, third_power, tuple(zero for _ in slots))

    weights = []
    for s in slots:
        moments = [halves(column(t)) for t in (*low_sums[s], *high_sums[s], top_sums[s])]
        weights.append(step_weights(moments, shifts[s]))

    rows = part.reshape(G * G, L)
    wide = stack_even.shape[1] // L

    def gathered(j, stack):
        for k in range(wide):
            y = wide * j + k
            total = None
            for s in slots:
                w = [c * u[s, y + 1, 8:72] for c, u in zip(weights[s], (u0, u1, u2))]
                term = (w[0] + w[1] + w[2]) * dens[s, y]
                total = term if total is None else total + term
            upper, lower = split(total)
            stack[0:G, k * L : k * L + L] = upper
            stack[G : 2 * G, k * L : k * L + L] = upper
            stack[2 * G : 3 * G, k * L : k * L + L] = lower

    def mixed(j, stack):
        sums = jnp.dot(kx, stack[...], preferred_element_type=F32)
        for k in range(wide):
            rows[pl.ds(wide * j + k, G, stride=G), :] = sums[:, k * L : k * L + L]

    gathered(0, stack_even)

    def finish(j, _):
        for stack, ahead, at in ((stack_even, stack_odd, 2 * j), (stack_odd, stack_even, 2 * j + 1)):
            gathered(lax.rem(at + 1, jnp.int32(G // wide)), ahead)
            mixed(at, stack)
        return 0

    for start, stop in bands:
        lax.fori_loop(start // (2 * wide), stop // (2 * wide), finish, 0)
        if after_band is not None:
            after_band(start)


def kernel(
    energies_in,
    frequencies_in,
    orbital_ids_in,
    freq_index_in,
    trials_in,
    orbitals,
    potential_in,
    coulomb_in,
    out,
    energies,
    frequencies,
    orbital_ids,
    freq_index,
    trials,
    potential,
    coulomb,
    input_sem,
    orbital_lines,
    orbital_sem,
    full,
    mapped,
    pot_other,
    dens,
    pot,
    u0,
    u1,
    u2,
    near_even,
    near_odd,
    stack_even,
    stack_odd,
    part,
    other,
    small,
    first_send,
    first_recv,
    second_send,
    second_recv,
    sum_send,
    sum_recv,
    pair_send,
    pair_recv,
    small_send,
    small_recv,
    *landing,
):
    me = Place()
    slots = range(dens.shape[0])
    half = lanes() < G

    inputs = [
        pltpu.make_async_copy(src, dst, input_sem.at[i])
        for i, (src, dst) in enumerate(
            (
                (trials_in, trials),
                (potential_in, potential),
                (coulomb_in, coulomb),
                (energies_in, energies),
                (frequencies_in, frequencies),
                (orbital_ids_in, orbital_ids),
                (freq_index_in, freq_index),
            )
        )
    ]
    for copy in inputs:
        copy.start()
    barrier = pltpu.get_barrier_semaphore()
    peers = [me.peer(a, by) for a in DIMS for by in (1, 2, 3)] + [me.partner()]
    for peer in peers:
        pl.semaphore_signal(barrier, inc=1, device_id=peer, device_id_type=MESH)

    orbital_copy = pltpu.make_async_copy(orbitals, orbital_lines, orbital_sem)
    orbital_copy.start()
    plane = me.own(full)
    for copy in inputs[:2]:
        copy.wait()
    for k in range(G // 2):
        a = trials[0, :, k * L : (k + 1) * L]
        b = trials[1, :, k * L : (k + 1) * L]
        plane[2 * k : 2 * k + 1, :] = jnp.where(half, a, swap(b))
        plane[2 * k + 1 : 2 * k + 2, :] = jnp.where(half, swap(a), b)
    for k in range(EXTRA):
        start = pl.multiple_of((me.trial * EXTRA + k) * L, L)
        plane[G + k : G + k + 1, :] = potential[:, pl.ds(start, L)]

    pl.semaphore_wait(barrier, len(peers))

    def prepare():
        def clear(y, _):
            for u in (u0, u1, u2):
                for s in slots:
                    u[s, y, 0:8] = jnp.zeros((8, L), F32)
                    u[s, y, 72:80] = jnp.zeros((8, L), F32)
            return 0

        for u in (u0, u1, u2):
            for s in slots:
                u[s, 0] = jnp.zeros((GROUP, L), F32)
                u[s, G + 1] = jnp.zeros((GROUP, L), F32)
        lax.fori_loop(1, G + 1, clear, 0)
        orbital_copy.wait()
        for copy in inputs[2:]:
            copy.wait()

        def spread_out(k, _):
            for s in slots:
                t = orbital_lines[s, :, pl.ds(pl.multiple_of(k * L, L), L)].astype(F32)
                turned = swap(t)
                dens[s, 2 * k] = jnp.where(half, t, turned)
                dens[s, 2 * k + 1] = jnp.where(half, turned, t)
            return 0

        lax.fori_loop(0, G // 2, spread_out, 0)

    full_rows = full.reshape(G * (G + EXTRA), L)
    other_rows = pot_other.reshape(G * EXTRA, L)
    mapped_rows = mapped.reshape(G * (G + SUMS), L)

    def level(j, base, t):
        turned = swap(t)
        y = 2 * (base + j)
        pot[y] = 2.0 * jnp.where(half, t, turned) - 2.0 * MID
        pot[y + 1] = 2.0 * jnp.where(half, turned, t) - 2.0 * MID

    def own_level(j, _):
        level(j, me.trial * EXTRA, full_rows[pl.ds(G + j, G, stride=G + EXTRA), :])
        return 0

    def other_level(j, _):
        level(j, (1 - me.trial) * EXTRA, other_rows[pl.ds(j, G, stride=EXTRA), :])
        return 0

    pot_copies = []

    def exchange_potential(color):
        if color == 0:
            lines = full.at[:, :, :, pl.ds(G, EXTRA)]
            pot_copies.append(remote(lines, pot_other, pair_send.at[0], pair_recv.at[0], me.partner()))
            lax.fori_loop(0, EXTRA, own_level, 0, unroll=4)

    sends = gather(me, full, FIRST_COLORS, first_send, first_recv, prepare, exchange_potential)
    (pot_copy,) = pot_copies

    def levels():
        pot_copy.wait_recv()
        lax.fori_loop(0, EXTRA, other_level, 0, unroll=4)

    shifts = []
    for s in slots:
        level_shift = frequencies[freq_index[s]] - energies[orbital_ids[s]]
        shifts.append(2.0 * (3.0 + level_shift) + 2.0 * MID)

    kx = coulomb[0]
    kx_upper = kx.astype(BF16)
    kx_lower = (kx - kx_upper.astype(F32)).astype(BF16)
    kx_parts = -jnp.concatenate([kx_upper, kx_lower, kx_upper], axis=1)
    kz = jnp.concatenate([coulomb[2], coulomb[2]], axis=1)
    kz = jnp.concatenate([kz, kz], axis=0)
    same = (lax.broadcasted_iota(jnp.int32, (L, L), 0) < G) == (lax.broadcasted_iota(jnp.int32, (L, L), 1) < G)
    kz = jnp.where(same, kz, 0.0)

    def in_plane(values):
        turned = lax.dot_general(
            values, kz, (((1,), (1,)), ((), ())), precision=HIGHEST, preferred_element_type=F32
        )
        return jnp.dot(coulomb[1], turned, precision=HIGHEST, preferred_element_type=F32)

    bands = [(rows.start, rows.start + rows.size) for _, rows in SUM_COLORS]
    fields = (u0, u1, u2, near_even, near_odd, stack_even, stack_odd)
    total = me.own(part)
    n = len(landing) // 2
    scatter = Scatter(me, part, landing[:n], SUM_COLORS, sum_send.at[0], sum_recv.at[0])
    respond(
        fields,
        dens,
        pot,
        shifts,
        kx_parts,
        part,
        lambda y: full_rows[pl.ds(y, G, stride=G + EXTRA), :],
        levels,
        bands,
        scatter.start,
    )
    part_sends = scatter.finish()
    own_mapped = in_plane(total[...])
    own_trials = plane[0:G, :]
    sums = me.own(mapped)
    sums[0:G, :] = own_mapped
    sums[G : G + 1, :] = column(fold(own_trials * own_trials))
    sums[G + 1 : G + 2, :] = column(fold(own_trials * own_mapped))
    sums[G + 2 : G + 3, :] = column(fold(own_mapped * own_mapped))
    sums[G + 3 : G + SUMS, :] = jnp.zeros((SUMS - 3, L), F32)
    sends += gather(me, mapped, SECOND_COLORS, second_send, second_recv)

    all_sums = jnp.zeros((SUMS, L), F32)
    for x in range(4):
        for z in range(4):
            for y in range(4):
                all_sums = all_sums + mapped[x, z, y, G : G + SUMS, :]
    squares = halves(all_sums[0:1])
    center = halves(all_sums[1:2]) / squares
    spread = jnp.sqrt(halves(all_sums[2:3]) / squares)
    unspread = 1.0 / spread

    def first_lines(y):
        t = full_rows[pl.ds(y, G, stride=G + EXTRA), :]
        m = mapped_rows[pl.ds(y, G, stride=G + SUMS), :]
        return (m - center * t) * unspread

    for copy in part_sends:
        copy.wait_send()
    scatter = Scatter(me, part, landing[n:], SUM_COLORS, sum_send.at[1], sum_recv.at[1])
    respond(fields, dens, pot, shifts, kx_parts, part, first_lines, None, bands, scatter.start)
    part_sends = scatter.finish()
    own_first = (own_mapped - center * own_trials) * unspread
    second = 2.0 * (in_plane(total[...]) - center * own_first) * unspread - own_trials

    other[0] = second
    swap_copy = remote(other.at[0], other.at[1], pair_send.at[1], pair_recv.at[1], me.partner())
    swap_copy.wait_recv()
    theirs = other[1]
    is_first = me.trial == 0
    a = jnp.where(is_first, second, theirs)
    b = jnp.where(is_first, theirs, second)
    turned_a = swap(a)
    turned_b = swap(b)
    place = lanes() % G
    row = jnp.zeros((1, L), F32)
    for k, product in enumerate((a * a, a * turned_a, b * b, b * turned_b, a * b, a * turned_b)):
        row = jnp.where(place == k, halves(column(fold(product))), row)
    small[me.orb] = row
    sends += part_sends + [pot_copy, swap_copy]
    everyone = small.shape[0]
    mine = small.at[me.orb]

    def tell(i, _):
        remote(
            mine, mine, small_send, small_recv, (lax.rem(me.orb + i, jnp.int32(everyone)), me.trial)
        )
        return 0

    lax.fori_loop(1, everyone, tell, 0)
    others = small.at[pl.ds(0, everyone - 1)]
    told = pltpu.make_async_remote_copy(
        src_ref=others,
        dst_ref=others,
        send_sem=small_send,
        recv_sem=small_recv,
        device_id=me.partner(),
        device_id_type=MESH,
    )
    told.wait_recv()
    sends.append(told)
    block = jnp.sum(small[...], axis=0) * (1.0 / float(G**3))

    def entry(k, upper):
        picked = jnp.where(lanes() == (k + G if upper else k), block, 0.0)
        return jnp.sum(picked, axis=1, keepdims=True)

    gram = {
        (0, 0): entry(0, False),
        (1, 1): entry(0, True),
        (1, 0): entry(1, False),
        (2, 2): entry(2, False),
        (3, 3): entry(2, True),
        (3, 2): entry(3, False),
        (2, 0): entry(4, False),
        (3, 1): entry(4, True),
        (3, 0): entry(5, False),
        (2, 1): entry(5, True),
    }
    lower = {}
    for j in range(4):
        rest = gram[j, j]
        for k in range(j):
            rest = rest - lower[j, k] * lower[j, k]
        lower[j, j] = jnp.sqrt(rest)
        for i in range(j + 1, 4):
            rest = gram[i, j]
            for k in range(j):
                rest = rest - lower[i, k] * lower[j, k]
            lower[i, j] = rest / lower[j, j]
    nothing = jnp.zeros((1, 1), F32)
    inverse = {(i, j): nothing for i in range(4) for j in range(4)}
    for j in range(4):
        inverse[j, j] = 1.0 / lower[j, j]
        for i in range(j + 1, 4):
            rest = nothing
            for k in range(j, i):
                rest = rest - lower[i, k] * inverse[k, j]
            inverse[i, j] = rest / lower[i, i]
    copies = (
        jnp.where(half, a, turned_a),
        jnp.where(half, turned_a, a),
        jnp.where(half, b, turned_b),
        jnp.where(half, turned_b, b),
    )
    result = None
    for u in range(4):
        here = jnp.where(is_first, inverse[0, u], inverse[2, u])
        there = jnp.where(is_first, inverse[1, u], inverse[3, u])
        term = jnp.where(half, here, there) * copies[u]
        result = term if result is None else result + term
    other[2] = result
    for k in range(G // 2):
        a = other[2, 2 * k : 2 * k + 1, :]
        b = other[2, 2 * k + 1 : 2 * k + 2, :]
        out[0, :, k * L : (k + 1) * L] = jnp.where(half, a, swap(b))
        out[1, :, k * L : (k + 1) * L] = jnp.where(half, swap(a), b)
    for copy in sends:
        copy.wait_send()


def shards(trials, orbitals, potential, coulomb, energies, frequencies, orbital_ids, freq_index):
    slots = orbitals.shape[0]
    vmem = pl.BlockSpec(memory_space=pltpu.VMEM)
    dma = pltpu.SemaphoreType.DMA
    field = pltpu.VMEM((slots, G + 2, GROUP, L), F32)
    near = pltpu.VMEM((slots, LINES, G, L), F32)
    stack = pltpu.VMEM((3 * G, WIDE * L), BF16)
    return pl.pallas_call(
        kernel,
        out_shape=jax.ShapeDtypeStruct(trials.shape, F32),
        in_specs=[pl.BlockSpec(memory_space=pl.ANY)] * 8,
        out_specs=vmem,
        scratch_shapes=[
            *(pltpu.SMEM(a.shape, a.dtype) for a in (energies, frequencies, orbital_ids, freq_index)),
            *(pltpu.VMEM(a.shape, a.dtype) for a in (trials, potential, coulomb)),
            dma((7,)),
            pltpu.VMEM(orbitals.shape, BF16),
            dma,
            pltpu.VMEM((4, 4, 4, G + EXTRA, L), F32),
            pltpu.VMEM((4, 4, 4, G + SUMS, L), F32),
            pltpu.VMEM((4, 4, 4, EXTRA, L), F32),
            pltpu.VMEM((slots, G, G, L), F32),
            pltpu.VMEM((G, G, L), F32),
            field,
            field,
            field,
            near,
            near,
            stack,
            stack,
            pltpu.VMEM((4, 4, 4, G, L), F32),
            pltpu.VMEM((3, G, L), F32),
            pltpu.VMEM((G, 1, L), F32),
            dma((3, 25)),
            dma((3, 25)),
            dma((3, 25)),
            dma((3, 25)),
            dma((2, 3, 18)),
            dma((2, 3, 18)),
            dma((2,)),
            dma((2,)),
            dma,
            dma,
            *landing_shapes(SUM_COLORS),
            *landing_shapes(SUM_COLORS),
        ],
        compiler_params=pltpu.CompilerParams(
            collective_id=0, has_side_effects=True, vmem_limit_bytes=60 * 2**20
        ),
        name="filter",
    )(energies, frequencies, orbital_ids, freq_index, trials, orbitals, potential, coulomb)


def solution(mesh):
    in_specs = (
        P("trial", "orb", None),
        P("orb", None, None),
        P("orb", None),
        P(),
        P(),
        P(),
        P("orb"),
        P("orb"),
    )
    return jax.shard_map(
        shards, mesh=mesh, in_specs=in_specs, out_specs=P("trial", "orb", None), check_vma=False
    )
```
